32 devices in a mesh: dp: 1 (over z), col: 4 (over y), row: 8 (over x, core).
Axes of the slice: x: 4, y: 4, z: 1, core: 2. Of those that a mesh axis runs over, the one named last changes fastest.
The devices are a block of a 4x4x8 slice.
Arguments:
- x_in: bfloat16 [2, 2048, 4096], P(None, ('dp', 'row'), 'col')
- ln_gamma: float32 [4096], P('col')
- w_in: bfloat16 [4096, 16384], P('row', 'col')
- w_out: bfloat16 [16384, 4096], P('row', 'col')
Outputs:
- output: bfloat16 [2, 2048, 4096], P(None, ('dp', 'row'), 'col')
All inputs are finite; a program needn't handle non-finite values.
Results may differ from the reference program's by a relative error of at most 0.001.
Values are sent between devices in bfloat16 or wider.
A program may use at most 768 MiB of HBM per device.

```python
import jax
import jax.numpy as jnp
from jax import lax

D_MODEL = 4096
D_FF = 16384
MB_TOKENS = 2048
ROW_BLOCK = 256
LN_EPS = 1e-5
N_BLOCKS = 2 * MB_TOKENS // ROW_BLOCK


def setup_inputs(seed: int = 0, part: int = 0) -> dict:
    base_key = jax.random.key(seed)
    part_key = jax.random.fold_in(base_key, part)
    key_noise, key_off, key_tilt, key_col = jax.random.split(part_key, 4)
    shared_key = jax.random.key(seed + 1)
    key_gamma, key_win, key_wout = jax.random.split(shared_key, 3)
    ramp = jnp.arange(D_MODEL, dtype=jnp.float32) / D_MODEL
    col_scale = (0.4 + 1.2 * ramp) * jax.random.uniform(key_col, (D_MODEL,), jnp.float32, 0.8, 1.2)
    noise = jax.random.normal(key_noise, (2, MB_TOKENS, D_MODEL), jnp.float32)
    row_off = 0.5 * jax.random.normal(key_off, (2, MB_TOKENS, 1), jnp.float32)
    row_tilt = jax.random.normal(key_tilt, (2, MB_TOKENS, 1), jnp.float32)
    x_val = row_off + row_tilt * (ramp - 0.5) + col_scale * noise
    ln_gamma = jax.random.uniform(key_gamma, (D_MODEL,), jnp.float32, 0.5, 1.5)
    w_in = jax.random.normal(key_win, (D_MODEL, D_FF), jnp.float32) * D_MODEL ** -0.5
    w_out = jax.random.normal(key_wout, (D_FF, D_MODEL), jnp.float32) * (1.5 * D_FF ** -0.5)
    return {"x_in": x_val.astype(jnp.bfloat16), "ln_gamma": ln_gamma, "w_in": w_in.astype(jnp.bfloat16), "w_out": w_out.astype(jnp.bfloat16)}


def reference(x_in, ln_gamma, w_in, w_out):
    row_blocks = x_in.reshape(N_BLOCKS, ROW_BLOCK, D_MODEL)

    def one_block(x_blk):
        x_f32 = x_blk.astype(jnp.float32)
        row_mean = jnp.sum(x_f32, axis=-1, keepdims=True) / D_MODEL
        row_var = jnp.sum(x_f32 * x_f32, axis=-1, keepdims=True) / D_MODEL - row_mean * row_mean
        z_norm = ((x_f32 - row_mean) * lax.rsqrt(row_var + LN_EPS) * ln_gamma).astype(jnp.bfloat16)
        hidden = jnp.dot(z_norm, w_in, preferred_element_type=jnp.float32)
        hidden = jax.nn.gelu(hidden, approximate=True).astype(jnp.bfloat16)
        branch = jnp.dot(hidden, w_out, preferred_element_type=jnp.float32)
        return (x_f32 + branch).astype(jnp.bfloat16)

    return lax.map(one_block, row_blocks).reshape(2, MB_TOKENS, D_MODEL)
```

```python
import functools

import jax
import jax.numpy as jnp
from jax import lax
from jax.experimental import pallas as pl
from jax.experimental.pallas import tpu as pltpu
from jax.sharding import PartitionSpec as P

LN_EPS = 1e-5
MESH = pl.DeviceIdType.MESH
CHUNKS = 4
N_SEMS = 144
GELU_C = 0.7978845608028654


class Comm:
    def __init__(self, send_sems, recv_sems, some_peer):
        self.send_sems, self.recv_sems, self.some_peer = send_sems, recv_sems, some_peer
        self.ids, self.sent = {}, []

    def _id(self, key):
        return self.ids.setdefault(key, len(self.ids))

    def send(self, key, src, dst, dev):
        i = self._id(key)
        copy = pltpu.make_async_remote_copy(
            src_ref=src, dst_ref=dst, send_sem=self.send_sems.at[i], recv_sem=self.recv_sems.at[i], device_id=dev, device_id_type=MESH
        )
        copy.start()
        self.sent.append(copy)

    def arrive(self, key, ref):
        i = self._id(key)
        pltpu.make_async_remote_copy(
            src_ref=ref, dst_ref=ref, send_sem=self.send_sems.at[i], recv_sem=self.recv_sems.at[i], device_id=self.some_peer, device_id_type=MESH
        ).wait_recv()

    def finish(self):
        for copy in self.sent:
            copy.wait_send()


def kernel(nx, ny, x_ref, gamma_ref, w1_ref, w2_ref, out_ref, xland, zb, w1b, w2b, hb, y0, yr, y1, gb, send_sems, recv_sems, loc_sems):
    T, D = x_ref.shape
    KR, FL = w1_ref.shape
    R2, N = w2_ref.shape
    FH = FL // 2
    FC = FH // CHUNKS
    NC = N // CHUNKS
    T2 = T // 2
    RH = R2 // 2

    row, y = lax.axis_index("row"), lax.axis_index("col")
    x, c = row // 2, row % 2
    xp, xi = nx - 1 - x, x + 1 - 2 * (x % 2)
    xf = nx - 1 - xi
    g = x // (nx // 2)
    up, dn, far = (y + 1) % ny, (y + ny - 1) % ny, (y + 2) % ny
    PX, PI, PC = {"row": 2 * xp + c}, {"row": 2 * xi + c}, {"row": 2 * x + 1 - c}
    YP, YM, YF = {"col": up}, {"col": dn}, {"col": far}

    barrier = pltpu.get_barrier_semaphore()
    for peer in (PX, PI, PC, YP, YM, YF):
        pl.semaphore_signal(barrier, inc=1, device_id=peer, device_id_type=MESH)
    pl.semaphore_wait(barrier, 6)

    comm = Comm(send_sems, recv_sems, PC)
    local = {}

    def local_copy(key, src, dst):
        copy = pltpu.make_async_copy(src, dst, loc_sems.at[len(local)])
        copy.start()
        local[key] = copy

    def tok(half):
        return pl.ds(half * T2, T2)

    def w1_src(grp, j):
        q, s = j // 2, j % 2
        col = pl.multiple_of(q * R2 + grp * RH + s * FC, FC)
        return w1_ref.at[:, pl.ds(col, FC)]

    def w1_dst(j, xx, cc):
        return w1b.at[j, pl.ds(pl.multiple_of((2 * xx + cc) * KR, KR), KR), :]

    def w2_src(grp, n):
        return w2_ref.at[pl.ds(pl.multiple_of(grp * RH, RH), RH), pl.ds(n * NC, NC)]

    def w2_dst(n, xx, cc):
        return w2b.at[n, pl.ds(pl.multiple_of((2 * xx + cc) * RH, RH), RH), :]

    def xl(h, yy, half):
        return xland.at[h, yy, tok(half), :]

    def hs(k, yy, half):
        h, j = divmod(k, CHUNKS)
        return hb.at[h, yy, tok(half), pl.ds(j * FC, FC)]

    for half in (0, 1):
        comm.send(("xp", half), x_ref.at[tok(half), :], xl(0, y, half), PX)
    for a, b in ((0, 1), (1, 0)):
        comm.send(("x1P", a), x_ref.at[tok(a), :], xl(1, y, a), YP)
        comm.send(("x1M", b), x_ref.at[tok(b), :], xl(1, y, b), YM)
    for j in range(CHUNKS):
        comm.send(("w1x", j), w1_src(1 - g, j), w1_dst(j, x, c), PX)
        comm.send(("w1i", j), w1_src(g, j), w1_dst(j, x, c), PI)
        comm.send(("w1c", 0, j), w1_src(g, j), w1_dst(j, x, c), PC)
        local_copy(("w1", j), w1_src(g, j), w1_dst(j, x, c))
    for yk, dev in (("P", YP), ("M", YM), ("F", YF)):
        comm.send(("g" + yk,), gamma_ref, gb.at[y], dev)
    local_copy("g", gamma_ref, gb.at[y])
    for n in range(CHUNKS):
        comm.send(("w2x", n), w2_src(1 - g, n), w2_dst(n, x, c), PX)
        comm.send(("w2c", 0, n), w2_src(g, n), w2_dst(n, x, c), PC)
        local_copy(("w2", n), w2_src(g, n), w2_dst(n, x, c))

    def w_from_inner(w, dst, j):
        comm.arrive((w + "i", j), dst(j, xi, c))
        comm.send((w + "c", 1, j), dst(j, xi, c), dst(j, xi, c), PC)

    def w_from_pair(w, dst, j):
        comm.arrive((w + "x", j), dst(j, xp, c))
        comm.send((w + "f", j), dst(j, xp, c), dst(j, xp, c), PI)
        comm.send((w + "c", 2, j), dst(j, xp, c), dst(j, xp, c), PC)

    def w_from_far(w, dst, j):
        comm.arrive((w + "f", j), dst(j, xf, c))
        comm.send((w + "c", 3, j), dst(j, xf, c), dst(j, xf, c), PC)

    def w_ready(w, dst, j):
        for i, xx in enumerate((x, xi, xp, xf)):
            comm.arrive((w + "c", i, j), dst(j, xx, 1 - c))
        local[(w, j)].wait()

    def x_load(h):
        if h == 0:
            local_copy(("z", h, 0), xland.at[0, y], zb.at[y])
        else:
            local_copy(("z", h, 0), x_ref, zb.at[y])
        for i, yy in enumerate((up, dn, far)):
            local_copy(("z", h, i + 1), xland.at[h, yy], zb.at[yy])
        for i in range(4):
            local[("z", h, i)].wait()

    def norm():
        rb = 32

        def body(i, carry):
            rows = pl.ds(pl.multiple_of(i * rb, rb), rb)
            s = jnp.zeros((rb, 1), jnp.float32)
            q = jnp.zeros((rb, 1), jnp.float32)
            for yy in range(ny):
                v = zb[yy, rows, :].astype(jnp.float32)
                s += jnp.sum(v, axis=-1, keepdims=True)
                q += jnp.sum(v * v, axis=-1, keepdims=True)
            mu = s / (ny * D)
            var = q / (ny * D) - mu * mu
            inv = lax.rsqrt(var + LN_EPS)
            for yy in range(ny):
                v = zb[yy, rows, :].astype(jnp.float32)
                zb[yy, rows, :] = ((v - mu) * inv * gb[yy]).astype(jnp.bfloat16)
            return carry

        lax.fori_loop(0, T // rb, body, 0)

    def hidden(k):
        h, j = divmod(k, CHUNKS)
        mb = T2

        def body(i, carry):
            rows = pl.ds(pl.multiple_of(i * mb, mb), mb)
            u = jnp.zeros((mb, FC), jnp.float32)
            for yy in range(ny):
                u += jnp.dot(zb[yy, rows, :], w1b[j, yy * D : (yy + 1) * D, :], preferred_element_type=jnp.float32)
            cdf = 0.5 * (1.0 + jnp.tanh(GELU_C * (u + 0.044715 * (u * u * u))))
            hb[h, y, rows, j * FC : (j + 1) * FC] = (u * cdf).astype(jnp.bfloat16)
            return carry

        lax.fori_loop(0, T // mb, body, 0)
        for a, b in ((0, 1), (1, 0)):
            comm.send(("hP", k, a), hs(k, y, a), hs(k, y, a), YP)
            comm.send(("hM", k, b), hs(k, y, b), hs(k, y, b), YM)

    def relay(k):
        comm.arrive(("hP", k, 0), hs(k, dn, 0))
        comm.send(("fP", k), hs(k, dn, 0), hs(k, dn, 0), YP)
        comm.arrive(("hM", k, 1), hs(k, up, 1))
        comm.send(("fM", k), hs(k, up, 1), hs(k, up, 1), YM)

    def h_ready(k):
        comm.arrive(("hP", k, 1), hs(k, dn, 1))
        comm.arrive(("hM", k, 0), hs(k, up, 0))

    def far_ready(k):
        comm.arrive(("fP", k), hs(k, far, 0))
        comm.arrive(("fM", k), hs(k, far, 1))

    def project(h, acc, n, yys, j0, j1, first):
        for yy in yys:
            lo, size = j0 * FC, (j1 - j0) * FC
            base = yy * FH + lo
            if not isinstance(base, int):
                base = pl.multiple_of(base, FC)
            d = jnp.dot(hb[h, yy, :, lo : lo + size], w2b[n, pl.ds(base, size), :], preferred_element_type=jnp.float32)
            if first:
                acc[n] = d
                first = False
            else:
                acc[n] += d

    def partial_out(n):
        w_ready("w2", w2_dst, n)
        project(0, y0, n, range(ny), 0, CHUNKS, True)
        comm.send(("y", n), y0.at[n], yr.at[n], PX)

    comm.arrive(("xp", 0), xl(0, y, 0))
    comm.send(("x0P", 0), xl(0, y, 0), xl(0, y, 0), YP)
    comm.arrive(("xp", 1), xl(0, y, 1))
    comm.send(("x0P", 1), xl(0, y, 1), xl(0, y, 1), YP)
    comm.send(("x0M", 1), xl(0, y, 1), xl(0, y, 1), YM)
    comm.send(("x0M", 0), xl(0, y, 0), xl(0, y, 0), YM)
    w_from_inner("w1", w1_dst, 0)
    for h in (0, 1):
        hk = "x%d" % h
        comm.arrive((hk + "P", 0), xl(h, dn, 0))
        comm.send((hk + "p",), xl(h, dn, 0), xl(h, dn, 0), YP)
        comm.arrive((hk + "M", 1), xl(h, up, 1))
        comm.send((hk + "m",), xl(h, up, 1), xl(h, up, 1), YM)
        w_from_pair("w1", w1_dst, h)
        w_from_inner("w1", w1_dst, h + 1)
    w_from_inner("w1", w1_dst, 3)
    w_from_pair("w1", w1_dst, 2)

    def x_ready(h):
        hk = "x%d" % h
        comm.arrive((hk + "P", 1), xl(h, dn, 1))
        comm.arrive((hk + "M", 0), xl(h, up, 0))
        comm.arrive((hk + "p",), xl(h, far, 0))
        comm.arrive((hk + "m",), xl(h, far, 1))

    local["g"].wait()
    for yk, yy in (("P", dn), ("M", up), ("F", far)):
        comm.arrive(("g" + yk,), gb.at[yy])
    x_ready(0)
    x_load(0)
    norm()

    def w2_inner(n):
        comm.send(("w2i", n), w2_src(g, n), w2_dst(n, x, c), PI)

    w_from_far("w1", w1_dst, 0)
    w_ready("w1", w1_dst, 0)
    hidden(0)
    w_from_pair("w1", w1_dst, 3)
    w2_inner(0)
    for k in (1, 2, 3):
        w_from_far("w1", w1_dst, k)
        w_ready("w1", w1_dst, k)
        hidden(k)
        w_from_pair("w2", w2_dst, k - 1)
        w2_inner(k)
        relay(k - 1)
    x_ready(1)
    x_load(1)
    norm()
    hidden(4)
    w_from_pair("w2", w2_dst, 3)
    w_from_inner("w2", w2_dst, 0)
    w_from_far("w2", w2_dst, 0)
    relay(3)
    hidden(5)
    w_from_inner("w2", w2_dst, 1)
    w_from_far("w2", w2_dst, 1)
    relay(4)
    for k in range(CHUNKS):
        h_ready(k)
        far_ready(k)
    partial_out(0)
    hidden(6)
    partial_out(1)
    w_from_inner("w2", w2_dst, 2)
    w_from_far("w2", w2_dst, 2)
    relay(5)
    hidden(7)
    partial_out(2)
    local_copy("xres", x_ref, zb.at[0])
    relay(6)
    w_from_inner("w2", w2_dst, 3)
    w_from_far("w2", w2_dst, 3)
    partial_out(3)
    for k in (4, 5):
        h_ready(k)
        far_ready(k)
    for n in range(CHUNKS):
        project(1, y1, n, range(ny), 0, 2, True)
    relay(7)
    h_ready(6)
    far_ready(6)
    for n in range(CHUNKS):
        project(1, y1, n, range(ny), 2, 3, False)
    h_ready(7)
    for n in range(CHUNKS):
        project(1, y1, n, (y, up, dn), 3, 4, False)
    local["xres"].wait()
    for n in range(CHUNKS):
        comm.arrive(("y", n), yr.at[n])
    far_ready(7)
    for n in range(CHUNKS):
        project(1, y1, n, (far,), 3, 4, False)
        cols = slice(n * NC, (n + 1) * NC)
        zb[1, :, cols] = (zb[0, :, cols].astype(jnp.float32) + (y1[n] + yr[n])).astype(jnp.bfloat16)
    local_copy("out", zb.at[1], out_ref)
    local["out"].wait()
    comm.finish()
    assert len(comm.ids) <= N_SEMS and len(local) <= 32


def solution(mesh):
    nx, ny = mesh.shape["row"] // 2, mesh.shape["col"]
    act_spec = P(None, ("dp", "row"), "col")

    def per_device(x_blk, gamma_blk, w_in_blk, w_out_blk):
        mbs, toks, D = x_blk.shape
        T = mbs * toks
        KR, FL = w_in_blk.shape
        R2, N = w_out_blk.shape
        bf16, f32 = jnp.bfloat16, jnp.float32
        any_spec = pl.BlockSpec(memory_space=pl.ANY)
        vmem_spec = pl.BlockSpec(memory_space=pltpu.VMEM)
        NC = N // CHUNKS
        flops = 2 * 2 * T * (ny * D) * (FL // 2) * 2
        out, _ = pl.pallas_call(
            functools.partial(kernel, nx, ny),
            out_shape=(jax.ShapeDtypeStruct((T, N), bf16), jax.ShapeDtypeStruct((2, ny, T, D), bf16)),
            in_specs=[any_spec, vmem_spec, any_spec, any_spec],
            out_specs=(any_spec, any_spec),
            scratch_shapes=[
                pltpu.VMEM((ny, T, D), bf16),
                pltpu.VMEM((CHUNKS, 2 * nx * KR, FL // 2 // CHUNKS), bf16),
                pltpu.VMEM((CHUNKS, nx * R2, NC), bf16),
                pltpu.VMEM((2, ny, T, FL // 2), bf16),
                pltpu.VMEM((CHUNKS, T, NC), f32),
                pltpu.VMEM((CHUNKS, T, NC), f32),
                pltpu.VMEM((CHUNKS, T, NC), f32),
                pltpu.VMEM((ny, 1, D), f32),
                pltpu.SemaphoreType.DMA((N_SEMS,)),
                pltpu.SemaphoreType.DMA((N_SEMS,)),
                pltpu.SemaphoreType.DMA((32,)),
            ],
            compiler_params=pltpu.CompilerParams(collective_id=0, has_side_effects=True, vmem_limit_bytes=67043328),
            cost_estimate=pl.CostEstimate(flops=flops, bytes_accessed=64 * T * D, transcendentals=T * FL),
            name="ln_mlp",
        )(x_blk.reshape(T, D), gamma_blk.reshape(1, D), w_in_blk, w_out_blk)
        return out.reshape(x_blk.shape)

    return jax.shard_map(per_device, mesh=mesh, in_specs=(act_spec, P("col"), P("row", "col"), P("row", "col")), out_specs=act_spec, check_vma=False)
```

```python
import functools

import jax
import jax.numpy as jnp
from jax import lax
from jax.experimental import pallas as pl
from jax.experimental.pallas import tpu as pltpu
from jax.sharding import PartitionSpec as P

LN_EPS = 1e-5
MESH = pl.DeviceIdType.MESH
CHUNKS = 4
N_SEMS = 160
GELU_C = 0.7978845608028654


class Comm:
    def __init__(self, send_sems, recv_sems, some_peer):
        self.send_sems, self.recv_sems, self.some_peer = send_sems, recv_sems, some_peer
        self.ids, self.sent = {}, []

    def _id(self, key):
        return self.ids.setdefault(key, len(self.ids))

    def send(self, key, src, dst, dev):
        i = self._id(key)
        copy = pltpu.make_async_remote_copy(
            src_ref=src, dst_ref=dst, send_sem=self.send_sems.at[i], recv_sem=self.recv_sems.at[i], device_id=dev, device_id_type=MESH
        )
        copy.start()
        self.sent.append(copy)

    def arrive(self, key, ref):
        i = self._id(key)
        pltpu.make_async_remote_copy(
            src_ref=ref, dst_ref=ref, send_sem=self.send_sems.at[i], recv_sem=self.recv_sems.at[i], device_id=self.some_peer, device_id_type=MESH
        ).wait_recv()

    def finish(self):
        for copy in self.sent:
            copy.wait_send()


def kernel(nx, ny, x_ref, gamma_ref, w1_ref, w2_ref, own_ref, got_ref, xland, zb, w1b, w2b, hb, y0, y1, gb, send_sems, recv_sems, loc_sems):
    T, D = x_ref.shape
    KR, FL = w1_ref.shape
    R2, N = w2_ref.shape
    FH = FL // 2
    FC = FH // CHUNKS
    NC = N // CHUNKS
    T2 = T // 2
    RH = R2 // 2
    T4 = T // 4
    pieces = [(n, 0, NC) for n in range(CHUNKS - 1)] + [(CHUNKS - 1, 0, NC // 2), (CHUNKS - 1, NC // 2, NC // 2)]
    seq = [(1, 0), (0, 0), (0, 1), (0, 2), (0, 3), (1, 1), (1, 2), (1, 3)]

    row, y = lax.axis_index("row"), lax.axis_index("col")
    x, c = row // 2, row % 2
    xp, xi = nx - 1 - x, x + 1 - 2 * (x % 2)
    xf = nx - 1 - xi
    g = x // (nx // 2)
    up, dn, far = (y + 1) % ny, (y + ny - 1) % ny, (y + 2) % ny
    PX, PI, PC = {"row": 2 * xp + c}, {"row": 2 * xi + c}, {"row": 2 * x + 1 - c}
    YP, YM, YF = {"col": up}, {"col": dn}, {"col": far}

    barrier = pltpu.get_barrier_semaphore()
    for peer in (PX, PI, PC, YP, YM, YF):
        pl.semaphore_signal(barrier, inc=1, device_id=peer, device_id_type=MESH)
    pl.semaphore_wait(barrier, 6)

    comm = Comm(send_sems, recv_sems, PC)
    local = {}

    def local_copy(key, src, dst):
        copy = pltpu.make_async_copy(src, dst, loc_sems.at[len(local)])
        copy.start()
        local[key] = copy

    def tok(half):
        return pl.ds(half * T2, T2)

    def w1_src(grp, j):
        q, s = j // 2, j % 2
        col = pl.multiple_of(q * R2 + grp * RH + s * FC, FC)
        return w1_ref.at[:, pl.ds(col, FC)]

    def w1_dst(j, xx, cc):
        return w1b.at[j, pl.ds(pl.multiple_of((2 * xx + cc) * KR, KR), KR), :]

    def w2_src(grp, p):
        n, lo, size = pieces[p]
        return w2_ref.at[pl.ds(pl.multiple_of(grp * RH, RH), RH), pl.ds(n * NC + lo, size)]

    def w2_dst(p, xx, cc):
        n, lo, size = pieces[p]
        return w2b.at[n, pl.ds(pl.multiple_of((2 * xx + cc) * RH, RH), RH), pl.ds(lo, size)]

    def xl(h, yy, half):
        return xland.at[h, yy, tok(half), :]

    def xq(h, yy, quarter):
        return xland.at[h, yy, pl.ds(quarter * T4, T4), :]

    def hs(k, yy, half):
        h, j = seq[k]
        return hb.at[h, yy, tok(half), pl.ds(j * FC, FC)]

    for quarter in (2, 0, 3, 1):
        comm.send(("xp", quarter), x_ref.at[pl.ds(quarter * T4, T4), :], xq(0, y, quarter), PX)
    for a, b in ((0, 1), (1, 0)):
        comm.send(("x1P", a), x_ref.at[tok(a), :], xl(1, y, a), YP)
        comm.send(("x1M", b), x_ref.at[tok(b), :], xl(1, y, b), YM)

    def w1_outer(j):
        comm.send(("w1x", j), w1_src(1 - g, j), w1_dst(j, x, c), PX)

    def w1_inner(j):
        comm.send(("w1i", j), w1_src(g, j), w1_dst(j, x, c), PI)

    def w2_inner(p):
        comm.send(("w2i", p), w2_src(g, p), w2_dst(p, x, c), PI)

    w1_outer(0)
    for j in (0, 1, 2):
        w1_inner(j)
    for j in range(CHUNKS):
        comm.send(("w1c", 0, j), w1_src(g, j), w1_dst(j, x, c), PC)
        local_copy(("w1", j), w1_src(g, j), w1_dst(j, x, c))
    for yk, dev in (("P", YP), ("M", YM), ("F", YF)):
        comm.send(("g" + yk,), gamma_ref, gb.at[y], dev)
    local_copy("g", gamma_ref, gb.at[y])
    for p in range(len(pieces)):
        comm.send(("w2c", 0, p), w2_src(g, p), w2_dst(p, x, c), PC)
        local_copy(("w2", p), w2_src(g, p), w2_dst(p, x, c))

    def w_from_inner(w, dst, j):
        comm.arrive((w + "i", j), dst(j, xi, c))
        comm.send((w + "c", 1, j), dst(j, xi, c), dst(j, xi, c), PC)

    def w_from_pair(w, dst, j):
        comm.arrive((w + "x", j), dst(j, xp, c))
        comm.send((w + "f", j), dst(j, xp, c), dst(j, xp, c), PI)
        comm.send((w + "c", 2, j), dst(j, xp, c), dst(j, xp, c), PC)

    def w_from_far(w, dst, j):
        comm.arrive((w + "f", j), dst(j, xf, c))
        comm.send((w + "c", 3, j), dst(j, xf, c), dst(j, xf, c), PC)

    def w_ready(w, dst, j):
        for i, xx in enumerate((x, xi, xp, xf)):
            comm.arrive((w + "c", i, j), dst(j, xx, 1 - c))
        local[(w, j)].wait()

    def x_load(h):
        local_copy(("z", h, 0), xland.at[0, y] if h == 0 else x_ref, zb.at[h, y])
        for i, yy in enumerate((up, dn, far)):
            local_copy(("z", h, i + 1), xland.at[h, yy], zb.at[h, yy])
        for i in range(4):
            local[("z", h, i)].wait()

    def norm(h):
        rb = 32

        def body(i, carry):
            rows = pl.ds(pl.multiple_of(i * rb, rb), rb)
            s = jnp.zeros((rb, 1), jnp.float32)
            q = jnp.zeros((rb, 1), jnp.float32)
            for yy in range(ny):
                v = zb[h, yy, rows, :].astype(jnp.float32)
                s += jnp.sum(v, axis=-1, keepdims=True)
                q += jnp.sum(v * v, axis=-1, keepdims=True)
            mu = s / (ny * D)
            var = q / (ny * D) - mu * mu
            inv = lax.rsqrt(var + LN_EPS)
            for yy in range(ny):
                v = zb[h, yy, rows, :].astype(jnp.float32)
                zb[h, yy, rows, :] = ((v - mu) * inv * gb[yy]).astype(jnp.bfloat16)
            return carry

        lax.fori_loop(0, T // rb, body, 0)

    def hidden(k):
        h, j = seq[k]
        mb = T2

        def body(i, carry):
            rows = pl.ds(pl.multiple_of(i * mb, mb), mb)
            u = jnp.zeros((mb, FC), jnp.float32)
            for yy in range(ny):
                u += jnp.dot(zb[h, yy, rows, :], w1b[j, yy * D : (yy + 1) * D, :], preferred_element_type=jnp.float32)
            cdf = 0.5 * (1.0 + jnp.tanh(GELU_C * (u + 0.044715 * (u * u * u))))
            hb[h, y, rows, j * FC : (j + 1) * FC] = (u * cdf).astype(jnp.bfloat16)
            return carry

        lax.fori_loop(0, T // mb, body, 0)
        for a, b in ((0, 1), (1, 0)):
            comm.send(("hP", k, a), hs(k, y, a), hs(k, y, a), YP)
            comm.send(("hM", k, b), hs(k, y, b), hs(k, y, b), YM)

    def relay(k):
        comm.arrive(("hP", k, 0), hs(k, dn, 0))
        comm.send(("fP", k), hs(k, dn, 0), hs(k, dn, 0), YP)
        comm.arrive(("hM", k, 1), hs(k, up, 1))
        comm.send(("fM", k), hs(k, up, 1), hs(k, up, 1), YM)

    def h_ready(k):
        comm.arrive(("hP", k, 1), hs(k, dn, 1))
        comm.arrive(("hM", k, 0), hs(k, up, 0))

    def far_ready(k):
        comm.arrive(("fP", k), hs(k, far, 0))
        comm.arrive(("fM", k), hs(k, far, 1))

    def project(h, acc, p, yys, j0, j1, first, rows=slice(None)):
        n, c0, size = pieces[p]
        cols = slice(c0, c0 + size)
        for yy in yys:
            lo, depth = j0 * FC, (j1 - j0) * FC
            base = yy * FH + lo
            if not isinstance(base, int):
                base = pl.multiple_of(base, FC)
            d = jnp.dot(hb[h, yy, rows, lo : lo + depth], w2b[n, pl.ds(base, depth), cols], preferred_element_type=jnp.float32)
            if first:
                acc[n, rows, cols] = d
                first = False
            else:
                acc[n, rows, cols] += d

    def got_at(p):
        n, c0, size = pieces[p]
        return got_ref.at[:, pl.ds(n * NC + c0, size)]

    def partial_out(p):
        n, c0, size = pieces[p]
        w_ready("w2", w2_dst, p)
        project(0, y0, p, range(ny), 0, CHUNKS, True)
        comm.send(("y", p), y0.at[n, :, pl.ds(c0, size)], got_at(p), PX)

    comm.arrive(("x1P", 0), xl(1, dn, 0))
    comm.send(("eP",), xl(1, dn, 0), xl(0, dn, 0), PX)
    comm.arrive(("x1M", 1), xl(1, up, 1))
    comm.send(("eM",), xl(1, up, 1), xl(0, up, 1), PX)
    for j in (1, 2, 3):
        w1_outer(j)
    for p in range(len(pieces)):
        comm.send(("w2x", p), w2_src(1 - g, p), w2_dst(p, x, c), PX)
    for quarter, dev in ((2, YP), (0, YM), (3, YP), (1, YM)):
        comm.arrive(("xp", quarter), xq(0, y, quarter))
        comm.send(("x0", quarter), xq(0, y, quarter), xq(0, y, quarter), dev)
    comm.send(("x1p",), xl(1, dn, 0), xl(1, dn, 0), YP)
    comm.send(("x1m",), xl(1, up, 1), xl(1, up, 1), YM)
    w_from_inner("w1", w1_dst, 0)
    w_from_inner("w1", w1_dst, 1)
    w_from_pair("w1", w1_dst, 0)
    w1_inner(3)
    w2_inner(0)
    for quarter in (2, 3):
        comm.arrive(("x0", quarter), xq(0, dn, quarter))
    comm.send(("x0p",), xl(0, dn, 1), xl(0, dn, 1), YP)
    for quarter in (0, 1):
        comm.arrive(("x0", quarter), xq(0, up, quarter))
    comm.send(("x0m",), xl(0, up, 0), xl(0, up, 0), YM)
    w_from_inner("w1", w1_dst, 2)

    local["g"].wait()
    for yk, yy in (("P", dn), ("M", up), ("F", far)):
        comm.arrive(("g" + yk,), gb.at[yy])
    comm.arrive(("x1P", 1), xl(1, dn, 1))
    comm.arrive(("x1M", 0), xl(1, up, 0))
    comm.arrive(("x1p",), xl(1, far, 0))
    comm.arrive(("x1m",), xl(1, far, 1))
    x_load(1)
    norm(1)
    w_from_far("w1", w1_dst, 0)
    w_ready("w1", w1_dst, 0)
    hidden(0)
    comm.arrive(("eP",), xl(0, dn, 0))
    comm.arrive(("eM",), xl(0, up, 1))
    comm.arrive(("x0p",), xl(0, far, 1))
    comm.arrive(("x0m",), xl(0, far, 0))
    x_load(0)
    norm(0)
    hidden(1)
    w_from_inner("w1", w1_dst, 3)
    w_from_pair("w1", w1_dst, 1)
    relay(0)
    w_from_pair("w1", w1_dst, 2)
    w_from_far("w1", w1_dst, 1)
    w_ready("w1", w1_dst, 1)
    hidden(2)
    relay(1)
    w_from_pair("w1", w1_dst, 3)
    w2_inner(1)
    w_from_far("w1", w1_dst, 2)
    w_ready("w1", w1_dst, 2)
    hidden(3)
    w_from_pair("w2", w2_dst, 0)
    relay(2)
    w_from_far("w1", w1_dst, 3)
    w_ready("w1", w1_dst, 3)
    hidden(4)
    w_from_pair("w2", w2_dst, 1)
    w2_inner(2)
    relay(3)
    hidden(5)
    w_from_pair("w2", w2_dst, 2)
    w2_inner(3)
    w_from_inner("w2", w2_dst, 0)
    w_from_far("w2", w2_dst, 0)
    w_from_pair("w2", w2_dst, 3)
    w2_inner(4)
    w_from_pair("w2", w2_dst, 4)
    relay(4)
    hidden(6)
    w_from_inner("w2", w2_dst, 1)
    w_from_far("w2", w2_dst, 1)
    for k in range(5):
        h_ready(k)
        far_ready(k)
    partial_out(0)
    partial_out(1)
    relay(5)
    hidden(7)
    w_from_inner("w2", w2_dst, 2)
    w_from_far("w2", w2_dst, 2)
    partial_out(2)
    relay(6)
    h_ready(5)
    far_ready(5)
    w_from_inner("w2", w2_dst, 3)
    w_from_far("w2", w2_dst, 3)
    partial_out(3)
    for p in (0, 1, 2):
        project(1, y1, p, range(ny), 0, 2, True)
    w_from_inner("w2", w2_dst, 4)
    w_from_far("w2", w2_dst, 4)
    partial_out(4)
    relay(7)
    for p in (3, 4):
        project(1, y1, p, range(ny), 0, 2, True)
    h_ready(6)
    far_ready(6)
    for p in range(len(pieces)):
        project(1, y1, p, range(ny), 2, 3, False)
    h_ready(7)
    for p in range(len(pieces)):
        project(1, y1, p, (y, up, dn), 3, 4, False)
    far_ready(7)
    for n in range(CHUNKS):
        for p, piece in enumerate(pieces):
            if piece[0] == n:
                project(1, y1, p, (far,), 3, 4, False)
        local_copy(("out", n), y1.at[n], own_ref.at[:, pl.ds(n * NC, NC)])
    for p in range(len(pieces)):
        comm.arrive(("y", p), got_at(p))
    for n in range(CHUNKS):
        local[("out", n)].wait()
    comm.finish()
    assert len(comm.ids) <= N_SEMS and len(local) <= 32


def solution(mesh):
    nx, ny = mesh.shape["row"] // 2, mesh.shape["col"]
    act_spec = P(None, ("dp", "row"), "col")

    def per_device(x_blk, gamma_blk, w_in_blk, w_out_blk):
        mbs, toks, D = x_blk.shape
        T = mbs * toks
        KR, FL = w_in_blk.shape
        R2, N = w_out_blk.shape
        bf16, f32 = jnp.bfloat16, jnp.float32
        any_spec = pl.BlockSpec(memory_space=pl.ANY)
        vmem_spec = pl.BlockSpec(memory_space=pltpu.VMEM)
        NC = N // CHUNKS
        flops = 2 * 2 * T * (ny * D) * (FL // 2) * 2
        own, got, _ = pl.pallas_call(
            functools.partial(kernel, nx, ny),
            out_shape=(jax.ShapeDtypeStruct((T, N), f32), jax.ShapeDtypeStruct((T, N), f32), jax.ShapeDtypeStruct((2, ny, T, D), bf16)),
            in_specs=[any_spec, vmem_spec, any_spec, any_spec],
            out_specs=(any_spec, any_spec, any_spec),
            scratch_shapes=[
                pltpu.VMEM((2, ny, T, D), bf16),
                pltpu.VMEM((CHUNKS, 2 * nx * KR, FL // 2 // CHUNKS), bf16),
                pltpu.VMEM((CHUNKS, nx * R2, NC), bf16),
                pltpu.VMEM((2, ny, T, FL // 2), bf16),
                pltpu.VMEM((CHUNKS, T, NC), f32),
                pltpu.VMEM((CHUNKS, T, NC), f32),
                pltpu.VMEM((ny, 1, D), f32),
                pltpu.SemaphoreType.DMA((N_SEMS,)),
                pltpu.SemaphoreType.DMA((N_SEMS,)),
                pltpu.SemaphoreType.DMA((32,)),
            ],
            compiler_params=pltpu.CompilerParams(collective_id=0, has_side_effects=True, vmem_limit_bytes=67043328),
            cost_estimate=pl.CostEstimate(flops=flops, bytes_accessed=64 * T * D, transcendentals=T * FL),
            name="ln_mlp",
        )(x_blk.reshape(T, D), gamma_blk.reshape(1, D), w_in_blk, w_out_blk)
        out = x_blk.reshape(T, D).astype(f32) + (own + got)
        return out.astype(bf16).reshape(x_blk.shape)

    return jax.shard_map(per_device, mesh=mesh, in_specs=(act_spec, P("col"), P("row", "col"), P("row", "col")), out_specs=act_spec, check_vma=False)
```

```python
import functools

import jax
import jax.numpy as jnp
from jax import lax
from jax.experimental import pallas as pl
from jax.experimental.pallas import tpu as pltpu
from jax.sharding import PartitionSpec as P

LN_EPS = 1e-5
MESH = pl.DeviceIdType.MESH
CHUNKS = 4
N_SEMS = 176
GELU_C = 0.7978845608028654


class Comm:
    def __init__(self, send_sems, recv_sems, some_peer):
        self.send_sems, self.recv_sems, self.some_peer = send_sems, recv_sems, some_peer
        self.ids, self.sent = {}, []

    def _id(self, key):
        return self.ids.setdefault(key, len(self.ids))

    def send(self, key, src, dst, dev):
        i = self._id(key)
        copy = pltpu.make_async_remote_copy(
            src_ref=src, dst_ref=dst, send_sem=self.send_sems.at[i], recv_sem=self.recv_sems.at[i], device_id=dev, device_id_type=MESH
        )
        copy.start()
        self.sent.append(copy)

    def arrive(self, key, ref):
        i = self._id(key)
        pltpu.make_async_remote_copy(
            src_ref=ref, dst_ref=ref, send_sem=self.send_sems.at[i], recv_sem=self.recv_sems.at[i], device_id=self.some_peer, device_id_type=MESH
        ).wait_recv()

    def finish(self):
        for copy in self.sent:
            copy.wait_send()


def kernel(nx, ny, x_ref, gamma_ref, w1_ref, w2_ref, out_ref, xland, zb, w1b, w2b, hb, y0, yr, y1, gb, send_sems, recv_sems, loc_sems):
    T, D = x_ref.shape
    KR, FL = w1_ref.shape
    R2, N = w2_ref.shape
    FH = FL // 2
    FC = FH // CHUNKS
    NC = N // CHUNKS
    T2 = T // 2
    RH = R2 // 2
    T4 = T // 4
    pieces = [(n, 0, NC) for n in range(CHUNKS - 1)] + [(CHUNKS - 1, 0, NC // 2), (CHUNKS - 1, NC // 2, NC // 2)]
    wpieces = [(j, 0, FC) for j in range(CHUNKS - 1)] + [(CHUNKS - 1, 0, FC // 2), (CHUNKS - 1, FC // 2, FC // 2)]
    NP = len(pieces)
    seq = [(h, j) for h in (0, 1) for j in range(CHUNKS)]

    row, y = lax.axis_index("row"), lax.axis_index("col")
    x, c = row // 2, row % 2
    xp, xi = nx - 1 - x, x + 1 - 2 * (x % 2)
    xf = nx - 1 - xi
    g = x // (nx // 2)
    up, dn, far = (y + 1) % ny, (y + ny - 1) % ny, (y + 2) % ny
    PX, PI, PC = {"row": 2 * xp + c}, {"row": 2 * xi + c}, {"row": 2 * x + 1 - c}
    YP, YM, YF = {"col": up}, {"col": dn}, {"col": far}

    barrier = pltpu.get_barrier_semaphore()
    for peer in (PX, PI, PC, YP, YM, YF):
        pl.semaphore_signal(barrier, inc=1, device_id=peer, device_id_type=MESH)
    pl.semaphore_wait(barrier, 6)

    comm = Comm(send_sems, recv_sems, PC)
    local = {}

    def local_copy(key, src, dst):
        copy = pltpu.make_async_copy(src, dst, loc_sems.at[len(local)])
        copy.start()
        local[key] = copy

    def tok(half):
        return pl.ds(half * T2, T2)

    def w1_src(grp, p):
        j, lo, size = wpieces[p]
        q, s = j // 2, j % 2
        col = pl.multiple_of(q * R2 + grp * RH + s * FC + lo, size)
        return w1_ref.at[:, pl.ds(col, size)]

    def w1_dst(p, xx, cc):
        j, lo, size = wpieces[p]
        return w1b.at[j, pl.ds(pl.multiple_of((2 * xx + cc) * KR, KR), KR), pl.ds(lo, size)]

    def w2_src(grp, p):
        n, lo, size = pieces[p]
        return w2_ref.at[pl.ds(pl.multiple_of(grp * RH, RH), RH), pl.ds(n * NC + lo, size)]

    def w2_dst(p, xx, cc):
        n, lo, size = pieces[p]
        return w2b.at[n, pl.ds(pl.multiple_of((2 * xx + cc) * RH, RH), RH), pl.ds(lo, size)]

    def xl(h, yy, half):
        return xland.at[h, yy, tok(half), :]

    def xq(h, yy, quarter):
        return xland.at[h, yy, pl.ds(quarter * T4, T4), :]

    def hs(k, yy, half):
        h, j = seq[k]
        return hb.at[h, yy, tok(half), pl.ds(j * FC, FC)]

    def w1_inner(p):
        comm.send(("w1i", p), w1_src(g, p), w1_dst(p, x, c), PI)

    def w2_inner(p):
        comm.send(("w2i", p), w2_src(g, p), w2_dst(p, x, c), PI)

    for quarter in (0, 2, 1, 3):
        comm.send(("xp", quarter), x_ref.at[pl.ds(quarter * T4, T4), :], xq(0, y, quarter), PX)
    comm.send(("x1P",), x_ref.at[tok(1), :], xl(1, y, 1), YP)
    comm.send(("x1M",), x_ref.at[tok(0), :], xl(1, y, 0), YM)
    for p in (0, 1, 2, 3):
        w1_inner(p)
    for p in range(NP):
        comm.send(("w1x", p), w1_src(1 - g, p), w1_dst(p, x, c), PX)

    def w_from_inner(w, dst, j):
        comm.arrive((w + "i", j), dst(j, xi, c))
        comm.send((w + "c", 1, j), dst(j, xi, c), dst(j, xi, c), PC)

    def w_from_pair(w, dst, j):
        comm.arrive((w + "x", j), dst(j, xp, c))
        comm.send((w + "f", j), dst(j, xp, c), dst(j, xp, c), PI)
        comm.send((w + "c", 2, j), dst(j, xp, c), dst(j, xp, c), PC)

    def w_from_far(w, dst, j):
        comm.arrive((w + "f", j), dst(j, xf, c))
        comm.send((w + "c", 3, j), dst(j, xf, c), dst(j, xf, c), PC)

    def w_ready(w, dst, j):
        for i, xx in enumerate((x, xi, xp, xf)):
            comm.arrive((w + "c", i, j), dst(j, xx, 1 - c))
        local[(w, j)].wait()

    def x_load(h):
        local_copy(("z", h, 0), xland.at[0, y] if h == 0 else x_ref, zb.at[y])
        for i, yy in enumerate((up, dn, far)):
            local_copy(("z", h, i + 1), xland.at[h, yy], zb.at[yy])
        for i in range(4):
            local[("z", h, i)].wait()

    def norm():
        rb = 32

        def body(i, carry):
            rows = pl.ds(pl.multiple_of(i * rb, rb), rb)
            s = jnp.zeros((rb, 1), jnp.float32)
            q = jnp.zeros((rb, 1), jnp.float32)
            for yy in range(ny):
                v = zb[yy, rows, :].astype(jnp.float32)
                s += jnp.sum(v, axis=-1, keepdims=True)
                q += jnp.sum(v * v, axis=-1, keepdims=True)
            mu = s / (ny * D)
            var = q / (ny * D) - mu * mu
            inv = lax.rsqrt(var + LN_EPS)
            for yy in range(ny):
                v = zb[yy, rows, :].astype(jnp.float32)
                zb[yy, rows, :] = ((v - mu) * inv * gb[yy]).astype(jnp.bfloat16)
            return carry

        lax.fori_loop(0, T // rb, body, 0)

    def hidden(k):
        h, j = seq[k]
        mb = T2

        def body(i, carry):
            rows = pl.ds(pl.multiple_of(i * mb, mb), mb)
            u = jnp.zeros((mb, FC), jnp.float32)
            for yy in range(ny):
                u += jnp.dot(zb[yy, rows, :], w1b[j, yy * D : (yy + 1) * D, :], preferred_element_type=jnp.float32)
            cdf = 0.5 * (1.0 + jnp.tanh(GELU_C * (u + 0.044715 * (u * u * u))))
            hb[h, y, rows, j * FC : (j + 1) * FC] = (u * cdf).astype(jnp.bfloat16)
            return carry

        lax.fori_loop(0, T // mb, body, 0)
        for a, b in ((0, 1), (1, 0)):
            comm.send(("hP", k, a), hs(k, y, a), hs(k, y, a), YP)
            comm.send(("hM", k, b), hs(k, y, b), hs(k, y, b), YM)

    def relay(k):
        comm.arrive(("hP", k, 0), hs(k, dn, 0))
        comm.send(("fP", k), hs(k, dn, 0), hs(k, dn, 0), YP)
        comm.arrive(("hM", k, 1), hs(k, up, 1))
        comm.send(("fM", k), hs(k, up, 1), hs(k, up, 1), YM)

    def h_ready(k):
        comm.arrive(("hP", k, 1), hs(k, dn, 1))
        comm.arrive(("hM", k, 0), hs(k, up, 0))

    def far_ready(k):
        comm.arrive(("fP", k), hs(k, far, 0))
        comm.arrive(("fM", k), hs(k, far, 1))

    def project(h, acc, n, yys, j0, j1, first, cols=slice(None)):
        for yy in yys:
            lo, depth = j0 * FC, (j1 - j0) * FC
            base = yy * FH + lo
            if not isinstance(base, int):
                base = pl.multiple_of(base, FC)
            d = jnp.dot(hb[h, yy, :, lo : lo + depth], w2b[n, pl.ds(base, depth), cols], preferred_element_type=jnp.float32)
            if first:
                acc[n, :, cols] = d
                first = False
            else:
                acc[n, :, cols] += d

    def partial_out(p):
        n, c0, size = pieces[p]
        cols = slice(c0, c0 + size)
        for i, xx in enumerate((x, xi, xp)):
            comm.arrive(("w2c", i, p), w2_dst(p, xx, 1 - c))
        local[("w2", p)].wait()
        project(0, y0, n, (x, xi, xp), 0, CHUNKS, True, cols)
        comm.arrive(("w2c", 3, p), w2_dst(p, xf, 1 - c))
        project(0, y0, n, (xf,), 0, CHUNKS, False, cols)
        comm.send(("y", p), y0.at[n, :, pl.ds(c0, size)], yr.at[n, :, pl.ds(c0, size)], PX)

    def x_relay(quarter):
        comm.arrive(("xp", quarter), xq(0, y, quarter))
        comm.send(("x0P", quarter), xq(0, y, quarter), xq(0, y, quarter), YP)
        comm.send(("x0M", quarter), xq(0, y, quarter), xq(0, y, quarter), YM)

    def x_up(quarter):
        comm.arrive(("x0P", quarter), xq(0, dn, quarter))
        comm.send(("x0p", quarter), xq(0, dn, quarter), xq(0, dn, quarter), YP)

    def x_down(quarter):
        comm.arrive(("x0M", quarter), xq(0, up, quarter))
        comm.send(("x0m", quarter), xq(0, up, quarter), xq(0, up, quarter), YM)

    x_relay(0)
    for yk, dev in (("P", YP), ("M", YM), ("F", YF)):
        comm.send(("g" + yk,), gamma_ref, gb.at[y], dev)
    local_copy("g", gamma_ref, gb.at[y])
    x_relay(2)
    for p in range(NP):
        comm.send(("w1c", 0, p), w1_src(g, p), w1_dst(p, x, c), PC)
        local_copy(("w1", p), w1_src(g, p), w1_dst(p, x, c))
    x_up(0)
    x_relay(1)
    x_down(2)
    x_relay(3)
    w_from_inner("w1", w1_dst, 0)
    w_from_inner("w1", w1_dst, 1)
    x_up(1)
    comm.send(("eP",), xl(0, dn, 0), xl(1, dn, 0), PX)
    comm.arrive(("x1P",), xl(1, dn, 1))
    comm.send(("x1p",), xl(1, dn, 1), xl(1, dn, 1), YP)
    x_down(3)
    comm.send(("eM",), xl(0, up, 1), xl(1, up, 1), PX)
    comm.arrive(("x1M",), xl(1, up, 0))
    comm.send(("x1m",), xl(1, up, 0), xl(1, up, 0), YM)
    w_from_pair("w1", w1_dst, 0)
    for p in range(NP):
        comm.send(("w2x", p), w2_src(1 - g, p), w2_dst(p, x, c), PX)
    w_from_inner("w1", w1_dst, 2)
    w_from_pair("w1", w1_dst, 1)
    w1_inner(4)
    w_from_inner("w1", w1_dst, 3)

    local["g"].wait()
    for yk, yy in (("P", dn), ("M", up), ("F", far)):
        comm.arrive(("g" + yk,), gb.at[yy])
    for quarter in (2, 3):
        comm.arrive(("x0P", quarter), xq(0, dn, quarter))
        comm.arrive(("x0m", quarter), xq(0, far, quarter))
    for quarter in (0, 1):
        comm.arrive(("x0M", quarter), xq(0, up, quarter))
        comm.arrive(("x0p", quarter), xq(0, far, quarter))
    x_load(0)
    norm()
    w_from_far("w1", w1_dst, 0)
    w_ready("w1", w1_dst, 0)
    hidden(0)
    for p in range(NP):
        comm.send(("w2c", 0, p), w2_src(g, p), w2_dst(p, x, c), PC)
        local_copy(("w2", p), w2_src(g, p), w2_dst(p, x, c))
    w_from_pair("w1", w1_dst, 2)
    w_from_far("w1", w1_dst, 1)
    w_ready("w1", w1_dst, 1)
    hidden(1)
    relay(0)
    w_from_pair("w1", w1_dst, 3)
    w_from_inner("w1", w1_dst, 4)
    w_from_pair("w1", w1_dst, 4)
    w2_inner(0)
    w2_inner(1)
    w_from_far("w1", w1_dst, 2)
    w_ready("w1", w1_dst, 2)
    hidden(2)
    relay(1)
    w_from_far("w1", w1_dst, 3)
    w_from_far("w1", w1_dst, 4)
    w_ready("w1", w1_dst, 3)
    w_ready("w1", w1_dst, 4)
    hidden(3)
    relay(2)
    comm.arrive(("eP",), xl(1, dn, 0))
    comm.arrive(("eM",), xl(1, up, 1))
    comm.arrive(("x1p",), xl(1, far, 1))
    comm.arrive(("x1m",), xl(1, far, 0))
    x_load(1)
    norm()
    hidden(4)
    w_from_pair("w2", w2_dst, 0)
    w_from_pair("w2", w2_dst, 1)
    w2_inner(2)
    relay(3)
    hidden(5)
    w_from_pair("w2", w2_dst, 2)
    w2_inner(3)
    w_from_inner("w2", w2_dst, 0)
    w_from_far("w2", w2_dst, 0)
    w_from_pair("w2", w2_dst, 3)
    w2_inner(4)
    relay(4)
    w_from_pair("w2", w2_dst, 4)
    hidden(6)
    w_from_inner("w2", w2_dst, 1)
    w_from_far("w2", w2_dst, 1)
    for k in range(4):
        h_ready(k)
        far_ready(k)
    partial_out(0)
    partial_out(1)
    relay(5)
    hidden(7)
    local_copy("xres", x_ref, zb.at[0])
    h_ready(4)
    far_ready(4)
    for n in (0, 1):
        project(1, y1, n, range(ny), 0, 1, True)
    w_from_inner("w2", w2_dst, 2)
    w_from_far("w2", w2_dst, 2)
    partial_out(2)
    relay(6)
    project(1, y1, 2, range(ny), 0, 1, True)
    h_ready(5)
    far_ready(5)
    w_from_inner("w2", w2_dst, 3)
    w_from_far("w2", w2_dst, 3)
    partial_out(3)
    for n in (0, 1, 2):
        project(1, y1, n, range(ny), 1, 2, False)
    w_from_inner("w2", w2_dst, 4)
    relay(7)
    w_from_far("w2", w2_dst, 4)
    partial_out(4)
    project(1, y1, 3, range(ny), 0, 2, True)
    h_ready(6)
    far_ready(6)
    for n in range(CHUNKS):
        project(1, y1, n, range(ny), 2, 3, False)
    h_ready(7)
    for n in range(CHUNKS):
        project(1, y1, n, (y, up, dn), 3, 4, False)
    local["xres"].wait()
    for p in range(NP):
        n, c0, size = pieces[p]
        comm.arrive(("y", p), yr.at[n, :, pl.ds(c0, size)])
    far_ready(7)
    for n in range(CHUNKS):
        project(1, y1, n, (far,), 3, 4, False)
        cols = slice(n * NC, (n + 1) * NC)
        zb[1, :, cols] = (zb[0, :, cols].astype(jnp.float32) + (y1[n] + yr[n])).astype(jnp.bfloat16)
        local_copy(("out", n), zb.at[1, :, pl.ds(n * NC, NC)], out_ref.at[:, pl.ds(n * NC, NC)])
    for n in range(CHUNKS):
        local[("out", n)].wait()
    comm.finish()
    assert len(comm.ids) <= N_SEMS and len(local) <= 32


def solution(mesh):
    nx, ny = mesh.shape["row"] // 2, mesh.shape["col"]
    act_spec = P(None, ("dp", "row"), "col")

    def per_device(x_blk, gamma_blk, w_in_blk, w_out_blk):
        mbs, toks, D = x_blk.shape
        T = mbs * toks
        KR, FL = w_in_blk.shape
        R2, N = w_out_blk.shape
        bf16, f32 = jnp.bfloat16, jnp.float32
        any_spec = pl.BlockSpec(memory_space=pl.ANY)
        vmem_spec = pl.BlockSpec(memory_space=pltpu.VMEM)
        NC = N // CHUNKS
        flops = 2 * 2 * T * (ny * D) * (FL // 2) * 2
        out, _ = pl.pallas_call(
            functools.partial(kernel, nx, ny),
            out_shape=(jax.ShapeDtypeStruct((T, N), bf16), jax.ShapeDtypeStruct((2, ny, T, D), bf16)),
            in_specs=[any_spec, vmem_spec, any_spec, any_spec],
            out_specs=(any_spec, any_spec),
            scratch_shapes=[
                pltpu.VMEM((ny, T, D), bf16),
                pltpu.VMEM((CHUNKS, 2 * nx * KR, FL // 2 // CHUNKS), bf16),
                pltpu.VMEM((CHUNKS, nx * R2, NC), bf16),
                pltpu.VMEM((2, ny, T, FL // 2), bf16),
                pltpu.VMEM((CHUNKS, T, NC), f32),
                pltpu.VMEM((CHUNKS, T, NC), f32),
                pltpu.VMEM((CHUNKS, T, NC), f32),
                pltpu.VMEM((ny, 1, D), f32),
                pltpu.SemaphoreType.DMA((N_SEMS,)),
                pltpu.SemaphoreType.DMA((N_SEMS,)),
                pltpu.SemaphoreType.DMA((32,)),
            ],
            compiler_params=pltpu.CompilerParams(collective_id=0, has_side_effects=True, vmem_limit_bytes=67043328),
            cost_estimate=pl.CostEstimate(flops=flops, bytes_accessed=64 * T * D, transcendentals=T * FL),
            name="ln_mlp",
        )(x_blk.reshape(T, D), gamma_blk.reshape(1, D), w_in_blk, w_out_blk)
        return out.reshape(x_blk.shape)

    return jax.shard_map(per_device, mesh=mesh, in_specs=(act_spec, P("col"), P("row", "col"), P("row", "col")), out_specs=act_spec, check_vma=False)
```

```python
import functools

import jax
import jax.numpy as jnp
from jax import lax
from jax.experimental import pallas as pl
from jax.experimental.pallas import tpu as pltpu
from jax.sharding import PartitionSpec as P

LN_EPS = 1e-5
MESH = pl.DeviceIdType.MESH
CHUNKS = 4
N_RECV, N_SEND, N_LOCAL = 91, 6, 15
GELU_C = 0.7978845608028654


def arrival(key):
    kind = key[0]
    if kind in ("gP", "gM", "gF"):
        return ("g",)
    if kind in ("w1c", "w2c"):
        return (kind, key[1] == 3 and kind == "w2c", key[2])
    if (kind == "x0P" and key[1] >= 2) or (kind == "x0M" and key[1] < 2) or kind in ("x0p", "x0m"):
        return ("x0",)
    if kind in ("x1p", "x1m", "eP", "eM"):
        return ("x1",)
    if (kind == "hP" and key[2] == 1) or (kind == "hM" and key[2] == 0):
        return ("h", key[1])
    if kind in ("fP", "fM"):
        return ("f", key[1])
    if kind == "y":
        return ("y",)
    return key


class Comm:
    def __init__(self, send_sems, recv_sems, some_peer):
        self.send_sems, self.recv_sems, self.some_peer = send_sems, recv_sems, some_peer
        self.recv_ids, self.send_ids = {}, {}

    def _copy(self, group, arr, src, dst, dev):
        i = self.send_ids.setdefault(group, len(self.send_ids))
        j = self.recv_ids.setdefault(arr, len(self.recv_ids))
        return pltpu.make_async_remote_copy(
            src_ref=src, dst_ref=dst, send_sem=self.send_sems.at[i], recv_sem=self.recv_sems.at[j], device_id=dev, device_id_type=MESH
        )

    def send(self, key, src, dst, dev):
        kind = key[0]
        group = kind[:2] if kind[0] == "w" else "h" if kind[0] in "hf" else "x" if kind[0] in "xe" else kind[0]
        self._copy(group, arrival(key), src, dst, dev).start()

    def arrive(self, arr, ref):
        self._copy("w1", arr, ref, ref, self.some_peer).wait_recv()

    def finish(self, group, ref):
        self._copy(group, ("y",), ref, ref, self.some_peer).wait_send()


def kernel(nx, ny, x_ref, gamma_ref, w1_ref, w2_ref, out_ref, xland, zb, w1b, w2b, hb, y0, yr, y1, gb, send_sems, recv_sems, loc_sems):
    T, D = x_ref.shape
    KR, FL = w1_ref.shape
    R2, N = w2_ref.shape
    FH = FL // 2
    FC = FH // CHUNKS
    NC = N // CHUNKS
    T2 = T // 2
    RH = R2 // 2
    T4 = T // 4
    pieces = [(0, 0, NC), (0, NC, NC), (1, 0, NC), (1, NC, NC // 2), (1, NC + NC // 2, NC // 2)]
    wpieces = [(j, 0, FC) for j in range(CHUNKS - 1)] + [(CHUNKS - 1, 0, FC // 2), (CHUNKS - 1, FC // 2, FC // 2)]
    NP = len(pieces)
    seq = [(h, j) for h in (0, 1) for j in range(CHUNKS)]

    row, y = lax.axis_index("row"), lax.axis_index("col")
    x, c = row // 2, row % 2
    xp, xi = nx - 1 - x, x + 1 - 2 * (x % 2)
    xf = nx - 1 - xi
    g = x // (nx // 2)
    up, dn, far = (y + 1) % ny, (y + ny - 1) % ny, (y + 2) % ny
    PX, PI, PC = {"row": 2 * xp + c}, {"row": 2 * xi + c}, {"row": 2 * x + 1 - c}
    YP, YM, YF = {"col": up}, {"col": dn}, {"col": far}

    barrier = pltpu.get_barrier_semaphore()
    for peer in (PX, PI, PC, YP, YM, YF):
        pl.semaphore_signal(barrier, inc=1, device_id=peer, device_id_type=MESH)
    pl.semaphore_wait(barrier, 6)

    comm = Comm(send_sems, recv_sems, PC)
    local = {}

    def local_copy(key, src, dst):
        copy = pltpu.make_async_copy(src, dst, loc_sems.at[local.setdefault(key, len(local))])
        copy.start()

    def local_wait(key, ref):
        pltpu.make_async_copy(ref, ref, loc_sems.at[local[key]]).wait()

    def tok(half):
        return pl.ds(half * T2, T2)

    def w1_src(grp, p):
        j, lo, size = wpieces[p]
        q, s = j // 2, j % 2
        col = pl.multiple_of(q * R2 + grp * RH + s * FC + lo, size)
        return w1_ref.at[:, pl.ds(col, size)]

    def w1_dst(p, xx, cc):
        j, lo, size = wpieces[p]
        return w1b.at[j, pl.ds(pl.multiple_of((2 * xx + cc) * KR, KR), KR), pl.ds(lo, size)]

    def w2_src(grp, p):
        n, lo, size = pieces[p]
        return w2_ref.at[pl.ds(pl.multiple_of(grp * RH, RH), RH), pl.ds(2 * n * NC + lo, size)]

    def w2_dst(p, xx, cc):
        n, lo, size = pieces[p]
        return w2b.at[n, pl.ds(pl.multiple_of((2 * xx + cc) * RH, RH), RH), pl.ds(lo, size)]

    def xl(h, yy, half):
        return xland.at[h, yy, tok(half), :]

    def xq(h, yy, quarter):
        return xland.at[h, yy, pl.ds(quarter * T4, T4), :]

    def hs(k, yy, half):
        h, j = seq[k]
        return hb.at[h, yy, tok(half), pl.ds(j * FC, FC)]

    def w1_inner(p):
        comm.send(("w1i", p), w1_src(g, p), w1_dst(p, x, c), PI)

    def w2_inner(p):
        comm.send(("w2i", p), w2_src(g, p), w2_dst(p, x, c), PI)

    for quarter in (0, 2, 1, 3):
        comm.send(("xp", quarter), x_ref.at[pl.ds(quarter * T4, T4), :], xq(0, y, quarter), PX)
    comm.send(("x1P",), x_ref.at[tok(1), :], xl(1, y, 1), YP)
    comm.send(("x1M",), x_ref.at[tok(0), :], xl(1, y, 0), YM)
    for p in (0, 1, 2, 3):
        w1_inner(p)
    for p in range(NP):
        comm.send(("w1x", p), w1_src(1 - g, p), w1_dst(p, x, c), PX)

    def w_from_inner(w, dst, j):
        comm.arrive((w + "i", j), dst(j, xi, c))
        comm.send((w + "c", 1, j), dst(j, xi, c), dst(j, xi, c), PC)

    def w_from_pair(w, dst, j):
        comm.arrive((w + "x", j), dst(j, xp, c))
        comm.send((w + "f", j), dst(j, xp, c), dst(j, xp, c), PI)
        comm.send((w + "c", 2, j), dst(j, xp, c), dst(j, xp, c), PC)

    def w_from_far(w, dst, j):
        comm.arrive((w + "f", j), dst(j, xf, c))
        comm.send((w + "c", 3, j), dst(j, xf, c), dst(j, xf, c), PC)

    def w1_ready(p):
        j, lo, size = wpieces[p]
        comm.arrive(("w1c", False, p), w1b.at[j, pl.ds(0, nx * KR), pl.ds(lo, size)])
        local_wait(("w1", p), w1_dst(p, x, c))

    def w2_ready(p):
        n, lo, size = pieces[p]
        comm.arrive(("w2c", False, p), w2b.at[n, pl.ds(0, (nx - 1) * RH), pl.ds(lo, size)])
        local_wait(("w2", p), w2_dst(p, x, c))

    def w2_far_ready(p):
        comm.arrive(("w2c", True, p), w2_dst(p, xf, 1 - c))

    def x_load(h):
        local_copy(("z", h), xland.at[0, y] if h == 0 else x_ref, zb.at[y])
        for yy in (up, dn, far):
            local_copy(("z", h), xland.at[h, yy], zb.at[yy])
        local_wait(("z", h), zb)

    def norm():
        rb = 32

        def body(i, carry):
            rows = pl.ds(pl.multiple_of(i * rb, rb), rb)
            s = jnp.zeros((rb, 1), jnp.float32)
            q = jnp.zeros((rb, 1), jnp.float32)
            for yy in range(ny):
                v = zb[yy, rows, :].astype(jnp.float32)
                s += jnp.sum(v, axis=-1, keepdims=True)
                q += jnp.sum(v * v, axis=-1, keepdims=True)
            mu = s / (ny * D)
            var = q / (ny * D) - mu * mu
            inv = lax.rsqrt(var + LN_EPS)
            for yy in range(ny):
                v = zb[yy, rows, :].astype(jnp.float32)
                zb[yy, rows, :] = ((v - mu) * inv * gb[yy]).astype(jnp.bfloat16)
            return carry

        lax.fori_loop(0, T // rb, body, 0)

    def hidden(k):
        h, j = seq[k]
        mb = T2

        def body(i, carry):
            rows = pl.ds(pl.multiple_of(i * mb, mb), mb)
            u = jnp.zeros((mb, FC), jnp.float32)
            for yy in range(ny):
                u += jnp.dot(zb[yy, rows, :], w1b[j, yy * D : (yy + 1) * D, :], preferred_element_type=jnp.float32)
            cdf = 0.5 * (1.0 + jnp.tanh(GELU_C * (u + 0.044715 * (u * u * u))))
            hb[h, y, rows, j * FC : (j + 1) * FC] = (u * cdf).astype(jnp.bfloat16)
            return carry

        lax.fori_loop(0, T // mb, body, 0)
        for a, b in ((0, 1), (1, 0)):
            comm.send(("hP", k, a), hs(k, y, a), hs(k, y, a), YP)
            comm.send(("hM", k, b), hs(k, y, b), hs(k, y, b), YM)

    def relay(k):
        comm.arrive(("hP", k, 0), hs(k, dn, 0))
        comm.send(("fP", k), hs(k, dn, 0), hs(k, dn, 0), YP)
        comm.arrive(("hM", k, 1), hs(k, up, 1))
        comm.send(("fM", k), hs(k, up, 1), hs(k, up, 1), YM)

    def h_ready(k):
        h, j = seq[k]
        comm.arrive(("h", k), hb.at[h, 0, :, pl.ds(j * FC, FC)])

    def far_ready(k):
        h, j = seq[k]
        comm.arrive(("f", k), hb.at[h, 0, :, pl.ds(j * FC, FC)])

    def project(h, acc, n, yys, j0, j1, first, cols=slice(None)):
        for yy in yys:
            lo, depth = j0 * FC, (j1 - j0) * FC
            base = yy * FH + lo
            if not isinstance(base, int):
                base = pl.multiple_of(base, FC)
            d = jnp.dot(hb[h, yy, :, lo : lo + depth], w2b[n, pl.ds(base, depth), cols], preferred_element_type=jnp.float32)
            if first:
                acc[n, :, cols] = d
                first = False
            else:
                acc[n, :, cols] += d

    def partial_send(p):
        n, lo, size = pieces[p]
        comm.send(("y", p), y0.at[n, :, pl.ds(lo, size)], yr.at[n, :, pl.ds(lo, size)], PX)

    def x_relay(quarter):
        comm.arrive(("xp", quarter), xq(0, y, quarter))
        comm.send(("x0P", quarter), xq(0, y, quarter), xq(0, y, quarter), YP)
        comm.send(("x0M", quarter), xq(0, y, quarter), xq(0, y, quarter), YM)

    def x_up(quarter):
        comm.arrive(("x0P", quarter), xq(0, dn, quarter))
        comm.send(("x0p", quarter), xq(0, dn, quarter), xq(0, dn, quarter), YP)

    def x_down(quarter):
        comm.arrive(("x0M", quarter), xq(0, up, quarter))
        comm.send(("x0m", quarter), xq(0, up, quarter), xq(0, up, quarter), YM)

    x_relay(0)
    for yk, dev in (("P", YP), ("M", YM), ("F", YF)):
        comm.send(("g" + yk,), gamma_ref, gb.at[y], dev)
    local_copy("g", gamma_ref, gb.at[y])
    x_relay(2)
    for p in range(NP):
        comm.send(("w1c", 0, p), w1_src(g, p), w1_dst(p, x, c), PC)
        local_copy(("w1", p), w1_src(g, p), w1_dst(p, x, c))
    x_up(0)
    x_relay(1)
    x_down(2)
    x_relay(3)
    w_from_inner("w1", w1_dst, 0)
    w_from_inner("w1", w1_dst, 1)
    x_up(1)
    comm.send(("eP",), xl(0, dn, 0), xl(1, dn, 0), PX)
    comm.arrive(("x1P",), xl(1, dn, 1))
    comm.send(("x1p",), xl(1, dn, 1), xl(1, dn, 1), YP)
    x_down(3)
    comm.send(("eM",), xl(0, up, 1), xl(1, up, 1), PX)
    comm.arrive(("x1M",), xl(1, up, 0))
    comm.send(("x1m",), xl(1, up, 0), xl(1, up, 0), YM)
    w_from_pair("w1", w1_dst, 0)
    for p in range(NP):
        comm.send(("w2x", p), w2_src(1 - g, p), w2_dst(p, x, c), PX)
    w_from_inner("w1", w1_dst, 2)
    w_from_pair("w1", w1_dst, 1)
    w1_inner(4)
    w_from_inner("w1", w1_dst, 3)

    local_wait("g", gb.at[y])
    comm.arrive(("g",), gb.at[pl.ds(0, ny - 1)])
    comm.arrive(("x0",), xland.at[0, pl.ds(0, 2)])
    x_load(0)
    norm()
    w_from_far("w1", w1_dst, 0)
    w1_ready(0)
    hidden(0)
    for p in range(NP):
        comm.send(("w2c", 0, p), w2_src(g, p), w2_dst(p, x, c), PC)
        local_copy(("w2", p), w2_src(g, p), w2_dst(p, x, c))
    w_from_pair("w1", w1_dst, 2)
    w_from_far("w1", w1_dst, 1)
    w1_ready(1)
    hidden(1)
    relay(0)
    w_from_pair("w1", w1_dst, 3)
    w_from_inner("w1", w1_dst, 4)
    w_from_pair("w1", w1_dst, 4)
    w2_inner(0)
    w2_inner(1)
    w_from_far("w1", w1_dst, 2)
    w1_ready(2)
    hidden(2)
    relay(1)
    w_from_far("w1", w1_dst, 3)
    w_from_far("w1", w1_dst, 4)
    w1_ready(3)
    w1_ready(4)
    hidden(3)
    relay(2)
    comm.arrive(("x1",), xland.at[1, pl.ds(0, 2)])
    x_load(1)
    norm()
    hidden(4)
    w_from_pair("w2", w2_dst, 0)
    w_from_pair("w2", w2_dst, 1)
    w2_inner(2)
    relay(3)
    hidden(5)
    w_from_pair("w2", w2_dst, 2)
    w2_inner(3)
    w2_inner(4)
    w_from_inner("w2", w2_dst, 0)
    w_from_far("w2", w2_dst, 0)
    w_from_pair("w2", w2_dst, 3)
    relay(4)
    w_from_pair("w2", w2_dst, 4)
    hidden(6)
    w_from_inner("w2", w2_dst, 1)
    w_from_far("w2", w2_dst, 1)
    for k in range(4):
        h_ready(k)
        far_ready(k)
    for p in (0, 1):
        w2_ready(p)
        w2_far_ready(p)
    project(0, y0, 0, range(ny), 0, CHUNKS, True)
    partial_send(0)
    partial_send(1)
    w_from_inner("w2", w2_dst, 2)
    relay(5)
    hidden(7)
    local_copy("xres", x_ref, zb.at[0])
    h_ready(4)
    far_ready(4)
    project(1, y1, 0, range(ny), 0, 1, True)
    w_from_far("w2", w2_dst, 2)
    w2_ready(2)
    project(0, y0, 1, (x, xi, xp), 0, CHUNKS, True, slice(0, NC))
    w2_far_ready(2)
    project(0, y0, 1, (xf,), 0, CHUNKS, False, slice(0, NC))
    partial_send(2)
    relay(6)
    w_from_inner("w2", w2_dst, 3)
    w_from_inner("w2", w2_dst, 4)
    h_ready(5)
    far_ready(5)
    project(1, y1, 0, range(ny), 1, 2, False)
    w2_ready(3)
    w2_ready(4)
    project(0, y0, 1, (x, xi, xp), 0, CHUNKS, True, slice(NC, 2 * NC))
    for p in (3, 4):
        if p == 4:
            relay(7)
        w_from_far("w2", w2_dst, p)
        w2_far_ready(p)
        n, lo, size = pieces[p]
        project(0, y0, 1, (xf,), 0, CHUNKS, False, slice(lo, lo + size))
        partial_send(p)
    project(1, y1, 1, range(ny), 0, 2, True)
    h_ready(6)
    far_ready(6)
    for n in (0, 1):
        project(1, y1, n, range(ny), 2, 3, False)
    h_ready(7)
    for n in (0, 1):
        project(1, y1, n, (y, up, dn), 3, 4, False)
    local_wait("xres", zb.at[0])
    comm.arrive(("y",), yr)
    far_ready(7)
    for n in (0, 1):
        project(1, y1, n, (far,), 3, 4, False)
        lo, size = 2 * n * NC, 2 * NC
        cols = slice(lo, lo + size)
        zb[1, :, cols] = (zb[0, :, cols].astype(jnp.float32) + (y1[n] + yr[n])).astype(jnp.bfloat16)
        local_copy("out", zb.at[1, :, pl.ds(lo, size)], out_ref.at[:, pl.ds(lo, size)])
    local_wait("out", out_ref)
    comm.finish("x", xland.at[:, :, pl.ds(0, T * 7 // 8), :])
    comm.finish("w1", w1b.at[:, pl.ds(0, (2 * nx - 1) * KR), :])
    comm.finish("w2", w2b.at[:, pl.ds(0, (2 * nx - 1) * RH), :])
    comm.finish("h", hb.at[:, pl.ds(0, ny - 1)])
    comm.finish("y", y0)
    comm.finish("g", gb.at[pl.ds(0, ny - 1)])
    assert len(comm.recv_ids) == N_RECV and len(comm.send_ids) == N_SEND and len(local) == N_LOCAL, (len(comm.recv_ids), len(comm.send_ids), len(local))


def solution(mesh):
    nx, ny = mesh.shape["row"] // 2, mesh.shape["col"]
    act_spec = P(None, ("dp", "row"), "col")

    def per_device(x_blk, gamma_blk, w_in_blk, w_out_blk):
        mbs, toks, D = x_blk.shape
        T = mbs * toks
        KR, FL = w_in_blk.shape
        R2, N = w_out_blk.shape
        bf16, f32 = jnp.bfloat16, jnp.float32
        any_spec = pl.BlockSpec(memory_space=pl.ANY)
        vmem_spec = pl.BlockSpec(memory_space=pltpu.VMEM)
        NC = N // CHUNKS
        flops = 2 * 2 * T * (ny * D) * (FL // 2) * 2
        out, _ = pl.pallas_call(
            functools.partial(kernel, nx, ny),
            out_shape=(jax.ShapeDtypeStruct((T, N), bf16), jax.ShapeDtypeStruct((2, ny, T, D), bf16)),
            in_specs=[any_spec, vmem_spec, any_spec, any_spec],
            out_specs=(any_spec, any_spec),
            scratch_shapes=[
                pltpu.VMEM((ny, T, D), bf16),
                pltpu.VMEM((CHUNKS, 2 * nx * KR, FL // 2 // CHUNKS), bf16),
                pltpu.VMEM((2, nx * R2, 2 * NC), bf16),
                pltpu.VMEM((2, ny, T, FL // 2), bf16),
                pltpu.VMEM((2, T, 2 * NC), f32),
                pltpu.VMEM((2, T, 2 * NC), f32),
                pltpu.VMEM((2, T, 2 * NC), f32),
                pltpu.VMEM((ny, 1, D), f32),
                pltpu.SemaphoreType.DMA((N_SEND,)),
                pltpu.SemaphoreType.DMA((N_RECV,)),
                pltpu.SemaphoreType.DMA((N_LOCAL,)),
            ],
            compiler_params=pltpu.CompilerParams(collective_id=0, has_side_effects=True, vmem_limit_bytes=67043328),
            cost_estimate=pl.CostEstimate(flops=flops, bytes_accessed=64 * T * D, transcendentals=T * FL),
            name="ln_mlp",
        )(x_blk.reshape(T, D), gamma_blk.reshape(1, D), w_in_blk, w_out_blk)
        return out.reshape(x_blk.shape)

    return jax.shard_map(per_device, mesh=mesh, in_specs=(act_spec, P("col"), P("row", "col"), P("row", "col")), out_specs=act_spec, check_vma=False)
```

```python
import functools

import jax
import jax.numpy as jnp
from jax import lax
from jax.experimental import pallas as pl
from jax.experimental.pallas import tpu as pltpu
from jax.sharding import PartitionSpec as P

LN_EPS = 1e-5
MESH = pl.DeviceIdType.MESH
CHUNKS = 4
N_RECV, N_SEND, N_LOCAL = 96, 6, 17
GELU_C = 0.7978845608028654


def arrival(key):
    kind = key[0]
    if kind in ("gP", "gM", "gF"):
        return ("g",)
    if kind in ("w1c", "w2c"):
        return (kind, key[1] == 3 and kind == "w2c", key[2])
    if (kind == "x0P" and key[1] >= 2) or (kind == "x0M" and key[1] < 2):
        return ("x0",)
    if kind in ("x0p", "x0m"):
        return ("x0f",)
    if kind in ("x1p", "x1m", "eP", "eM"):
        return ("x1",)
    if (kind == "hP" and key[2] == 1) or (kind == "hM" and key[2] == 0):
        return ("h", key[1])
    if kind in ("fP", "fM"):
        return ("f", key[1])
    if kind == "y":
        return ("y",)
    return key


class Comm:
    def __init__(self, send_sems, recv_sems, some_peer):
        self.send_sems, self.recv_sems, self.some_peer = send_sems, recv_sems, some_peer
        self.recv_ids, self.send_ids = {}, {}

    def _copy(self, group, arr, src, dst, dev):
        i = self.send_ids.setdefault(group, len(self.send_ids))
        j = self.recv_ids.setdefault(arr, len(self.recv_ids))
        return pltpu.make_async_remote_copy(
            src_ref=src, dst_ref=dst, send_sem=self.send_sems.at[i], recv_sem=self.recv_sems.at[j], device_id=dev, device_id_type=MESH
        )

    def send(self, key, src, dst, dev):
        kind = key[0]
        group = kind[:2] if kind[0] == "w" else "h" if kind[0] in "hf" else "x" if kind[0] in "xe" else kind[0]
        self._copy(group, arrival(key), src, dst, dev).start()

    def arrive(self, arr, ref):
        self._copy("w1", arr, ref, ref, self.some_peer).wait_recv()

    def finish(self, group, ref):
        self._copy(group, ("y",), ref, ref, self.some_peer).wait_send()


def kernel(nx, ny, x_ref, gamma_ref, w1_ref, w2_ref, out_ref, xland, zb, w1b, w2b, hb, y0, yr, y1, gb, send_sems, recv_sems, loc_sems):
    T, D = x_ref.shape
    KR, FL = w1_ref.shape
    R2, N = w2_ref.shape
    FH = FL // 2
    FC = FH // CHUNKS
    NC = N // CHUNKS
    T2 = T // 2
    RH = R2 // 2
    T4 = T // 4
    pieces = [(0, 0, NC), (0, NC, NC), (1, 0, NC), (1, NC, NC // 2), (1, NC + NC // 2, NC // 2)]
    wpieces = [(0, 0, FC // 2), (0, FC // 2, FC // 2), (1, 0, FC), (2, 0, FC), (3, 0, FC // 2), (3, FC // 2, FC // 2)]
    NP, NW = len(pieces), len(wpieces)
    seq = [(h, j) for h in (0, 1) for j in range(CHUNKS)]

    row, y = lax.axis_index("row"), lax.axis_index("col")
    x, c = row // 2, row % 2
    xp, xi = nx - 1 - x, x + 1 - 2 * (x % 2)
    xf = nx - 1 - xi
    g = x // (nx // 2)
    up, dn, far = (y + 1) % ny, (y + ny - 1) % ny, (y + 2) % ny
    PX, PI, PC = {"row": 2 * xp + c}, {"row": 2 * xi + c}, {"row": 2 * x + 1 - c}
    YP, YM, YF = {"col": up}, {"col": dn}, {"col": far}

    barrier = pltpu.get_barrier_semaphore()
    for peer in (PX, PI, PC, YP, YM, YF):
        pl.semaphore_signal(barrier, inc=1, device_id=peer, device_id_type=MESH)
    pl.semaphore_wait(barrier, 6)

    comm = Comm(send_sems, recv_sems, PC)
    local = {}

    def local_copy(key, src, dst):
        copy = pltpu.make_async_copy(src, dst, loc_sems.at[local.setdefault(key, len(local))])
        copy.start()

    def local_wait(key, ref):
        pltpu.make_async_copy(ref, ref, loc_sems.at[local[key]]).wait()

    def tok(half):
        return pl.ds(half * T2, T2)

    def w1_src(grp, p):
        j, lo, size = wpieces[p]
        q, s = j // 2, j % 2
        col = pl.multiple_of(q * R2 + grp * RH + s * FC + lo, size)
        return w1_ref.at[:, pl.ds(col, size)]

    def w1_dst(p, xx, cc):
        j, lo, size = wpieces[p]
        return w1b.at[j, pl.ds(pl.multiple_of((2 * xx + cc) * KR, KR), KR), pl.ds(lo, size)]

    def w2_src(grp, p):
        n, lo, size = pieces[p]
        return w2_ref.at[pl.ds(pl.multiple_of(grp * RH, RH), RH), pl.ds(2 * n * NC + lo, size)]

    def w2_dst(p, xx, cc):
        n, lo, size = pieces[p]
        return w2b.at[n, pl.ds(pl.multiple_of((2 * xx + cc) * RH, RH), RH), pl.ds(lo, size)]

    def xl(h, yy, half):
        return xland.at[h, yy, tok(half), :]

    def xl_all(h):
        return xland.at[h, 0]

    def xq(h, yy, quarter):
        return xland.at[h, yy, pl.ds(quarter * T4, T4), :]

    def hs(k, yy, half):
        h, j = seq[k]
        return hb.at[h, yy, tok(half), pl.ds(j * FC, FC)]

    def w1_inner(p):
        comm.send(("w1i", p), w1_src(g, p), w1_dst(p, x, c), PI)

    def w2_inner(p):
        comm.send(("w2i", p), w2_src(g, p), w2_dst(p, x, c), PI)

    for quarter in (0, 2, 1, 3):
        comm.send(("xp", quarter), x_ref.at[pl.ds(quarter * T4, T4), :], xq(0, y, quarter), PX)
    comm.send(("x1P",), x_ref.at[tok(1), :], xl(1, y, 1), YP)
    comm.send(("x1M",), x_ref.at[tok(0), :], xl(1, y, 0), YM)
    for p in range(4):
        w1_inner(p)
    for p in range(NW):
        comm.send(("w1x", p), w1_src(1 - g, p), w1_dst(p, x, c), PX)

    def w_from_inner(w, dst, j):
        comm.arrive((w + "i", j), dst(j, xi, c))
        comm.send((w + "c", 1, j), dst(j, xi, c), dst(j, xi, c), PC)

    def w_from_pair(w, dst, j):
        comm.arrive((w + "x", j), dst(j, xp, c))
        comm.send((w + "f", j), dst(j, xp, c), dst(j, xp, c), PI)
        comm.send((w + "c", 2, j), dst(j, xp, c), dst(j, xp, c), PC)

    def w_from_far(w, dst, j):
        comm.arrive((w + "f", j), dst(j, xf, c))
        comm.send((w + "c", 3, j), dst(j, xf, c), dst(j, xf, c), PC)

    def w1_ready(p):
        j, lo, size = wpieces[p]
        comm.arrive(("w1c", False, p), w1b.at[j, pl.ds(0, nx * KR), pl.ds(lo, size)])
        local_wait(("w1", p), w1_dst(p, x, c))

    def w2_ready(p):
        n, lo, size = pieces[p]
        comm.arrive(("w2c", False, p), w2b.at[n, pl.ds(0, (nx - 1) * RH), pl.ds(lo, size)])
        local_wait(("w2", p), w2_dst(p, x, c))

    def w2_far_ready(p):
        comm.arrive(("w2c", True, p), w2_dst(p, xf, 1 - c))

    def x_load(key, h, blocks):
        for yy in blocks:
            local_copy(("z", h, key), xland.at[h, yy], zb.at[yy])

    def x_loaded(key, h, count):
        local_wait(("z", h, key), zb.at[pl.ds(0, count)])

    def norm():
        rb = 32

        def body(i, carry):
            rows = pl.ds(pl.multiple_of(i * rb, rb), rb)
            s = jnp.zeros((rb, 1), jnp.float32)
            q = jnp.zeros((rb, 1), jnp.float32)
            for yy in range(ny):
                v = zb[yy, rows, :].astype(jnp.float32)
                s += jnp.sum(v, axis=-1, keepdims=True)
                q += jnp.sum(v * v, axis=-1, keepdims=True)
            mu = s / (ny * D)
            var = q / (ny * D) - mu * mu
            inv = lax.rsqrt(var + LN_EPS)
            for yy in range(ny):
                v = zb[yy, rows, :].astype(jnp.float32)
                zb[yy, rows, :] = ((v - mu) * inv * gb[yy]).astype(jnp.bfloat16)
            return carry

        lax.fori_loop(0, T // rb, body, 0)

    def hidden_part(j, rows, blocks):
        u = None
        for yy in blocks:
            base = yy * D
            if not isinstance(base, int):
                base = pl.multiple_of(base, D)
            d = jnp.dot(zb[yy, rows, :], w1b[j, pl.ds(base, D), :], preferred_element_type=jnp.float32)
            u = d if u is None else u + d
        return u

    def hidden_store(h, j, rows, u):
        cdf = 0.5 * (1.0 + jnp.tanh(GELU_C * (u + 0.044715 * (u * u * u))))
        hb[h, y, rows, j * FC : (j + 1) * FC] = (u * cdf).astype(jnp.bfloat16)

    def hidden_send(k, a, b):
        comm.send(("hP", k, a), hs(k, y, a), hs(k, y, a), YP)
        comm.send(("hM", k, b), hs(k, y, b), hs(k, y, b), YM)

    def hidden(k):
        h, j = seq[k]

        def body(i, carry):
            rows = pl.ds(pl.multiple_of(i * T2, T2), T2)
            hidden_store(h, j, rows, hidden_part(j, rows, range(ny)))
            return carry

        lax.fori_loop(0, 2, body, 0)
        hidden_send(k, 0, 1)
        hidden_send(k, 1, 0)

    def relay(k):
        comm.arrive(("hP", k, 0), hs(k, dn, 0))
        comm.send(("fP", k), hs(k, dn, 0), hs(k, dn, 0), YP)
        comm.arrive(("hM", k, 1), hs(k, up, 1))
        comm.send(("fM", k), hs(k, up, 1), hs(k, up, 1), YM)

    def h_ready(k):
        h, j = seq[k]
        comm.arrive(("h", k), hb.at[h, 0, :, pl.ds(j * FC, FC)])

    def far_ready(k):
        h, j = seq[k]
        comm.arrive(("f", k), hb.at[h, 0, :, pl.ds(j * FC, FC)])

    def project(h, acc, n, start, count, j0, j1, cols=slice(None), first=False):
        lo, depth = j0 * FC, (j1 - j0) * FC

        def body(i, carry):
            rows = pl.ds(pl.multiple_of(i * T2, T2), T2)
            total = None
            for b in range(count):
                yy = (start + b) % ny
                base = yy * FH + lo
                if not isinstance(base, int):
                    base = pl.multiple_of(base, FC)
                d = jnp.dot(hb[h, yy, rows, lo : lo + depth], w2b[n, pl.ds(base, depth), cols], preferred_element_type=jnp.float32)
                total = d if total is None else total + d
            acc[n, rows, cols] = total if first else acc[n, rows, cols] + total
            return carry

        lax.fori_loop(0, 2, body, 0)

    def partial_send(p):
        n, lo, size = pieces[p]
        comm.send(("y", p), y0.at[n, :, pl.ds(lo, size)], yr.at[n, :, pl.ds(lo, size)], PX)

    def early(p):
        n, lo, size = pieces[p]
        w2_ready(p)
        project(0, y0, n, xf + 1, ny - 1, 0, CHUNKS, slice(lo, lo + size), first=True)

    def late(p):
        n, lo, size = pieces[p]
        w2_far_ready(p)
        project(0, y0, n, xf, 1, 0, CHUNKS, slice(lo, lo + size))
        partial_send(p)

    def x_relay(quarter):
        comm.arrive(("xp", quarter), xq(0, y, quarter))
        comm.send(("x0P", quarter), xq(0, y, quarter), xq(0, y, quarter), YP)
        comm.send(("x0M", quarter), xq(0, y, quarter), xq(0, y, quarter), YM)

    def x_up(quarter):
        comm.arrive(("x0P", quarter), xq(0, dn, quarter))
        comm.send(("x0p", quarter), xq(0, dn, quarter), xq(0, dn, quarter), YP)

    def x_down(quarter):
        comm.arrive(("x0M", quarter), xq(0, up, quarter))
        comm.send(("x0m", quarter), xq(0, up, quarter), xq(0, up, quarter), YM)

    x_relay(0)
    for yk, dev in (("P", YP), ("M", YM), ("F", YF)):
        comm.send(("g" + yk,), gamma_ref, gb.at[y], dev)
    local_copy("g", gamma_ref, gb.at[y])
    x_relay(2)
    for p in range(NW):
        comm.send(("w1c", 0, p), w1_src(g, p), w1_dst(p, x, c), PC)
        local_copy(("w1", p), w1_src(g, p), w1_dst(p, x, c))
    x_up(0)
    x_relay(1)
    x_down(2)
    x_relay(3)
    w_from_inner("w1", w1_dst, 0)
    w_from_inner("w1", w1_dst, 1)
    w_from_pair("w1", w1_dst, 0)
    x_up(1)
    comm.send(("eP",), xl(0, dn, 0), xl(1, dn, 0), PX)
    comm.arrive(("x1P",), xl(1, dn, 1))
    comm.send(("x1p",), xl(1, dn, 1), xl(1, dn, 1), YP)
    w_from_pair("w1", w1_dst, 1)
    w1_inner(4)
    x_down(3)
    comm.send(("eM",), xl(0, up, 1), xl(1, up, 1), PX)
    comm.arrive(("x1M",), xl(1, up, 0))
    comm.send(("x1m",), xl(1, up, 0), xl(1, up, 0), YM)
    for p in range(NP):
        comm.send(("w2x", p), w2_src(1 - g, p), w2_dst(p, x, c), PX)
    w_from_inner("w1", w1_dst, 2)
    w_from_inner("w1", w1_dst, 3)
    w_from_far("w1", w1_dst, 0)
    w_from_pair("w1", w1_dst, 2)
    w_from_far("w1", w1_dst, 1)

    local_wait("g", gb.at[y])
    comm.arrive(("g",), gb.at[pl.ds(0, ny - 1)])
    comm.arrive(("x0",), xl_all(0))
    x_load("near", 0, (y, up, dn))
    comm.arrive(("x0f",), xl_all(0))
    x_load("far", 0, (far,))
    x_loaded("near", 0, ny - 1)
    x_loaded("far", 0, 1)
    norm()
    w1_ready(0)
    w1_ready(1)
    hidden(0)
    for p in range(NP):
        comm.send(("w2c", 0, p), w2_src(g, p), w2_dst(p, x, c), PC)
        local_copy(("w2", p), w2_src(g, p), w2_dst(p, x, c))
    w_from_pair("w1", w1_dst, 3)
    w1_inner(5)
    w_from_inner("w1", w1_dst, 4)
    w_from_far("w1", w1_dst, 2)
    relay(0)
    w1_ready(2)
    hidden(1)
    w_from_pair("w1", w1_dst, 4)
    w_from_pair("w1", w1_dst, 5)
    w2_inner(0)
    w2_inner(1)
    w_from_far("w1", w1_dst, 3)
    w1_ready(3)
    hidden(2)
    w_from_inner("w1", w1_dst, 5)
    relay(1)
    w_from_far("w1", w1_dst, 4)
    w_from_far("w1", w1_dst, 5)
    w1_ready(4)
    w1_ready(5)
    hidden(3)
    relay(2)
    comm.arrive(("x1",), xland.at[1, pl.ds(0, 2)])
    local_copy(("z", 1, "near"), x_ref, zb.at[y])
    x_load("near", 1, (up, dn, far))
    x_loaded("near", 1, ny)
    norm()
    hidden(4)
    w_from_pair("w2", w2_dst, 0)
    w_from_pair("w2", w2_dst, 1)
    w2_inner(2)
    relay(3)
    hidden(5)
    w_from_pair("w2", w2_dst, 2)
    w2_inner(3)
    w_from_inner("w2", w2_dst, 0)
    w_from_far("w2", w2_dst, 0)
    w_from_pair("w2", w2_dst, 3)
    w2_inner(4)
    relay(4)
    w_from_pair("w2", w2_dst, 4)
    w_from_inner("w2", w2_dst, 1)
    for k in range(4):
        h_ready(k)
    for k in range(3):
        far_ready(k)
    w2_ready(0)
    w2_far_ready(0)
    w_from_far("w2", w2_dst, 1)
    w2_ready(1)
    w2_far_ready(1)
    project(0, y0, 0, dn, ny - 1, 0, CHUNKS, first=True)
    project(0, y0, 0, far, 1, 0, CHUNKS - 1)
    far_ready(3)
    project(0, y0, 0, far, 1, CHUNKS - 1, CHUNKS)
    partial_send(0)
    partial_send(1)
    hidden(6)
    w_from_inner("w2", w2_dst, 2)
    relay(5)
    hidden(7)
    local_copy("xres", x_ref, zb.at[0])
    h_ready(4)
    far_ready(4)
    project(1, y1, 0, 0, ny, 0, 1, first=True)
    w_from_far("w2", w2_dst, 2)
    early(2)
    late(2)
    w_from_inner("w2", w2_dst, 3)
    relay(6)
    early(3)
    w_from_far("w2", w2_dst, 3)
    late(3)
    h_ready(5)
    far_ready(5)
    project(1, y1, 0, 0, ny, 1, 2)
    w_from_inner("w2", w2_dst, 4)
    early(4)
    relay(7)
    w_from_far("w2", w2_dst, 4)
    late(4)
    project(1, y1, 1, 0, ny, 0, 2, first=True)
    h_ready(6)
    h_ready(7)
    for n in (0, 1):
        project(1, y1, n, dn, ny - 1, 2, 4)
    far_ready(6)
    for n in (0, 1):
        project(1, y1, n, far, 1, 2, 3)
    local_wait("xres", zb.at[0])
    comm.arrive(("y",), yr)
    for n in (0, 1):
        y1[n] = y1[n] + yr[n] + zb[0, :, 2 * n * NC : 2 * (n + 1) * NC].astype(jnp.float32)
    far_ready(7)
    for n in (0, 1):
        cols = pl.ds(2 * n * NC, 2 * NC)
        base = pl.multiple_of(far * FH + 3 * FC, FC)
        for half in (0, 1):
            rows = slice(half * T2, (half + 1) * T2)
            last = jnp.dot(hb[1, far, rows, 3 * FC :], w2b[n, pl.ds(base, FC), :], preferred_element_type=jnp.float32)
            zb[1, rows, 2 * n * NC : 2 * (n + 1) * NC] = (y1[n, rows, :] + last).astype(jnp.bfloat16)
            local_copy("out", zb.at[1, tok(half), cols], out_ref.at[tok(half), cols])
    local_wait("out", out_ref)
    comm.finish("x", xland.at[:, :, pl.ds(0, T * 7 // 8), :])
    comm.finish("w1", w1b.at[:, pl.ds(0, (2 * nx - 1) * KR), :])
    comm.finish("w2", w2b.at[:, pl.ds(0, (2 * nx - 1) * RH), :])
    comm.finish("h", hb.at[:, pl.ds(0, ny - 1)])
    comm.finish("y", y0)
    comm.finish("g", gb.at[pl.ds(0, ny - 1)])
    assert len(comm.recv_ids) == N_RECV and len(comm.send_ids) == N_SEND and len(local) == N_LOCAL, (len(comm.recv_ids), len(comm.send_ids), len(local))


def solution(mesh):
    nx, ny = mesh.shape["row"] // 2, mesh.shape["col"]
    act_spec = P(None, ("dp", "row"), "col")

    def per_device(x_blk, gamma_blk, w_in_blk, w_out_blk):
        mbs, toks, D = x_blk.shape
        T = mbs * toks
        KR, FL = w_in_blk.shape
        R2, N = w_out_blk.shape
        bf16, f32 = jnp.bfloat16, jnp.float32
        any_spec = pl.BlockSpec(memory_space=pl.ANY)
        vmem_spec = pl.BlockSpec(memory_space=pltpu.VMEM)
        NC = N // CHUNKS
        flops = 2 * 2 * T * (ny * D) * (FL // 2) * 2
        out, _ = pl.pallas_call(
            functools.partial(kernel, nx, ny),
            out_shape=(jax.ShapeDtypeStruct((T, N), bf16), jax.ShapeDtypeStruct((2, ny, T, D), bf16)),
            in_specs=[any_spec, vmem_spec, any_spec, any_spec],
            out_specs=(any_spec, any_spec),
            scratch_shapes=[
                pltpu.VMEM((ny, T, D), bf16),
                pltpu.VMEM((CHUNKS, 2 * nx * KR, FL // 2 // CHUNKS), bf16),
                pltpu.VMEM((2, nx * R2, 2 * NC), bf16),
                pltpu.VMEM((2, ny, T, FL // 2), bf16),
                pltpu.VMEM((2, T, 2 * NC), f32),
                pltpu.VMEM((2, T, 2 * NC), f32),
                pltpu.VMEM((2, T, 2 * NC), f32),
                pltpu.VMEM((ny, 1, D), f32),
                pltpu.SemaphoreType.DMA((N_SEND,)),
                pltpu.SemaphoreType.DMA((N_RECV,)),
                pltpu.SemaphoreType.DMA((N_LOCAL,)),
            ],
            compiler_params=pltpu.CompilerParams(collective_id=0, has_side_effects=True, vmem_limit_bytes=67043328),
            cost_estimate=pl.CostEstimate(flops=flops, bytes_accessed=64 * T * D, transcendentals=T * FL),
            name="ln_mlp",
        )(x_blk.reshape(T, D), gamma_blk.reshape(1, D), w_in_blk, w_out_blk)
        return out.reshape(x_blk.shape)

    return jax.shard_map(per_device, mesh=mesh, in_specs=(act_spec, P("col"), P("row", "col"), P("row", "col")), out_specs=act_spec, check_vma=False)
```

```python
import functools

import jax
import jax.numpy as jnp
from jax import lax
from jax.experimental import pallas as pl
from jax.experimental.pallas import tpu as pltpu
from jax.sharding import PartitionSpec as P

LN_EPS = 1e-5
MESH = pl.DeviceIdType.MESH
CHUNKS = 4
N_RECV, N_SEND, N_LOCAL = 96, 6, 17
GELU_C = 0.7978845608028654


def arrival(key):
    kind = key[0]
    if kind in ("gP", "gM", "gF"):
        return ("g",)
    if kind in ("w1c", "w2c"):
        return (kind, key[1] == 3 and kind == "w2c", key[2])
    if (kind == "x0P" and key[1] >= 2) or (kind == "x0M" and key[1] < 2):
        return ("x0",)
    if kind in ("x0p", "x0m"):
        return ("x0f",)
    if kind in ("x1p", "x1m", "eP", "eM", "eF"):
        return ("x1",)
    if (kind == "hP" and key[2] == 1) or (kind == "hM" and key[2] == 0):
        return ("h", key[1])
    if kind in ("fP", "fM"):
        return ("f", key[1])
    if kind == "y":
        return ("y",)
    return key


class Comm:
    def __init__(self, send_sems, recv_sems, some_peer):
        self.send_sems, self.recv_sems, self.some_peer = send_sems, recv_sems, some_peer
        self.recv_ids, self.send_ids = {}, {}

    def _copy(self, group, arr, src, dst, dev):
        i = self.send_ids.setdefault(group, len(self.send_ids))
        j = self.recv_ids.setdefault(arr, len(self.recv_ids))
        return pltpu.make_async_remote_copy(
            src_ref=src, dst_ref=dst, send_sem=self.send_sems.at[i], recv_sem=self.recv_sems.at[j], device_id=dev, device_id_type=MESH
        )

    def send(self, key, src, dst, dev):
        kind = key[0]
        group = kind[:2] if kind[0] == "w" else "h" if kind[0] in "hf" else "x" if kind[0] in "xe" else kind[0]
        self._copy(group, arrival(key), src, dst, dev).start()

    def arrive(self, arr, ref):
        self._copy("w1", arr, ref, ref, self.some_peer).wait_recv()

    def finish(self, group, ref):
        self._copy(group, ("y",), ref, ref, self.some_peer).wait_send()


def kernel(nx, ny, x_ref, gamma_ref, w1_ref, w2_ref, out_ref, xland, zb, w1b, w2b, hb, y0, yr, y1, gb, send_sems, recv_sems, loc_sems):
    T, D = x_ref.shape
    KR, FL = w1_ref.shape
    R2, N = w2_ref.shape
    FH = FL // 2
    FC = FH // CHUNKS
    NC = N // CHUNKS
    T2 = T // 2
    RH = R2 // 2
    T4, T8 = T // 4, T // 8
    pieces = [(0, 0, NC), (0, NC, NC), (1, 0, NC), (1, NC, NC // 2), (1, NC + NC // 2, NC // 2)]
    wpieces = [(0, 0, FC // 2), (0, FC // 2, FC // 2), (1, 0, FC), (2, 0, FC), (3, 0, FC // 2), (3, FC // 2, FC // 2)]
    NP, NW = len(pieces), len(wpieces)
    seq = [(h, j) for h in (0, 1) for j in range(CHUNKS)]

    row, y = lax.axis_index("row"), lax.axis_index("col")
    x, c = row // 2, row % 2
    xp, xi = nx - 1 - x, x + 1 - 2 * (x % 2)
    xf = nx - 1 - xi
    g = x // (nx // 2)
    up, dn, far = (y + 1) % ny, (y + ny - 1) % ny, (y + 2) % ny
    PX, PI, PC = {"row": 2 * xp + c}, {"row": 2 * xi + c}, {"row": 2 * x + 1 - c}
    YP, YM, YF = {"col": up}, {"col": dn}, {"col": far}

    barrier = pltpu.get_barrier_semaphore()
    for peer in (PX, PI, PC, YP, YM, YF):
        pl.semaphore_signal(barrier, inc=1, device_id=peer, device_id_type=MESH)
    pl.semaphore_wait(barrier, 6)

    comm = Comm(send_sems, recv_sems, PC)
    local = {}

    def local_copy(key, src, dst):
        copy = pltpu.make_async_copy(src, dst, loc_sems.at[local.setdefault(key, len(local))])
        copy.start()

    def local_wait(key, ref):
        pltpu.make_async_copy(ref, ref, loc_sems.at[local[key]]).wait()

    def tok(half):
        return pl.ds(half * T2, T2)

    def w1_src(grp, p):
        j, lo, size = wpieces[p]
        q, s = j // 2, j % 2
        col = pl.multiple_of(q * R2 + grp * RH + s * FC + lo, size)
        return w1_ref.at[:, pl.ds(col, size)]

    def w1_dst(p, xx, cc):
        j, lo, size = wpieces[p]
        return w1b.at[j, pl.ds(pl.multiple_of((2 * xx + cc) * KR, KR), KR), pl.ds(lo, size)]

    def w2_src(grp, p):
        n, lo, size = pieces[p]
        return w2_ref.at[pl.ds(pl.multiple_of(grp * RH, RH), RH), pl.ds(2 * n * NC + lo, size)]

    def w2_dst(p, xx, cc):
        n, lo, size = pieces[p]
        return w2b.at[n, pl.ds(pl.multiple_of((2 * xx + cc) * RH, RH), RH), pl.ds(lo, size)]

    def xl(h, yy, half):
        return xland.at[h, yy, tok(half), :]

    def xs(h, yy, first, count):
        return xland.at[h, yy, pl.ds(first, count), :]

    def xl_all(h):
        return xland.at[h, 0]

    def xq(h, yy, quarter):
        return xland.at[h, yy, pl.ds(quarter * T4, T4), :]

    def hs(k, yy, half):
        h, j = seq[k]
        return hb.at[h, yy, tok(half), pl.ds(j * FC, FC)]

    def w1_inner(p):
        comm.send(("w1i", p), w1_src(g, p), w1_dst(p, x, c), PI)

    def w2_inner(p):
        comm.send(("w2i", p), w2_src(g, p), w2_dst(p, x, c), PI)

    for quarter in (0, 2, 1, 3):
        comm.send(("xp", quarter), x_ref.at[pl.ds(quarter * T4, T4), :], xq(0, y, quarter), PX)
    comm.send(("x1P",), x_ref.at[tok(1), :], xl(1, y, 1), YP)
    comm.send(("x1M",), x_ref.at[tok(0), :], xl(1, y, 0), YM)
    for p in range(4):
        w1_inner(p)
    for p in range(NW):
        comm.send(("w1x", p), w1_src(1 - g, p), w1_dst(p, x, c), PX)

    def w_from_inner(w, dst, j):
        comm.arrive((w + "i", j), dst(j, xi, c))
        comm.send((w + "c", 1, j), dst(j, xi, c), dst(j, xi, c), PC)

    def w_from_pair(w, dst, j):
        comm.arrive((w + "x", j), dst(j, xp, c))
        comm.send((w + "f", j), dst(j, xp, c), dst(j, xp, c), PI)
        comm.send((w + "c", 2, j), dst(j, xp, c), dst(j, xp, c), PC)

    def w_from_far(w, dst, j):
        comm.arrive((w + "f", j), dst(j, xf, c))
        comm.send((w + "c", 3, j), dst(j, xf, c), dst(j, xf, c), PC)

    def w1_ready(p):
        j, lo, size = wpieces[p]
        comm.arrive(("w1c", False, p), w1b.at[j, pl.ds(0, nx * KR), pl.ds(lo, size)])
        local_wait(("w1", p), w1_dst(p, x, c))

    def w2_ready(p):
        n, lo, size = pieces[p]
        comm.arrive(("w2c", False, p), w2b.at[n, pl.ds(0, (nx - 1) * RH), pl.ds(lo, size)])
        local_wait(("w2", p), w2_dst(p, x, c))

    def w2_far_ready(p):
        comm.arrive(("w2c", True, p), w2_dst(p, xf, 1 - c))

    def x_load(key, h, blocks):
        for yy in blocks:
            local_copy(("z", h, key), xland.at[h, yy], zb.at[yy])

    def x_loaded(key, h, count):
        local_wait(("z", h, key), zb.at[pl.ds(0, count)])

    def norm():
        rb = 32

        def body(i, carry):
            rows = pl.ds(pl.multiple_of(i * rb, rb), rb)
            s = jnp.zeros((rb, 1), jnp.float32)
            q = jnp.zeros((rb, 1), jnp.float32)
            for yy in range(ny):
                v = zb[yy, rows, :].astype(jnp.float32)
                s += jnp.sum(v, axis=-1, keepdims=True)
                q += jnp.sum(v * v, axis=-1, keepdims=True)
            mu = s / (ny * D)
            var = q / (ny * D) - mu * mu
            inv = lax.rsqrt(var + LN_EPS)
            for yy in range(ny):
                v = zb[yy, rows, :].astype(jnp.float32)
                zb[yy, rows, :] = ((v - mu) * inv * gb[yy]).astype(jnp.bfloat16)
            return carry

        lax.fori_loop(0, T // rb, body, 0)

    def hidden_part(j, rows, blocks):
        u = None
        for yy in blocks:
            base = yy * D
            if not isinstance(base, int):
                base = pl.multiple_of(base, D)
            d = jnp.dot(zb[yy, rows, :], w1b[j, pl.ds(base, D), :], preferred_element_type=jnp.float32)
            u = d if u is None else u + d
        return u

    def hidden_store(h, j, rows, u):
        cdf = 0.5 * (1.0 + jnp.tanh(GELU_C * (u + 0.044715 * (u * u * u))))
        hb[h, y, rows, j * FC : (j + 1) * FC] = (u * cdf).astype(jnp.bfloat16)

    def hidden_send(k, a, b):
        comm.send(("hP", k, a), hs(k, y, a), hs(k, y, a), YP)
        comm.send(("hM", k, b), hs(k, y, b), hs(k, y, b), YM)

    def hidden(k):
        h, j = seq[k]

        def body(i, carry):
            rows = pl.ds(pl.multiple_of(i * T2, T2), T2)
            hidden_store(h, j, rows, hidden_part(j, rows, range(ny)))
            return carry

        if k == 0:
            body(0, 0)
            comm.send(("hP", k, 0), hs(k, y, 0), hs(k, y, 0), YP)
            body(1, 0)
            comm.send(("hM", k, 1), hs(k, y, 1), hs(k, y, 1), YM)
            hidden_send(k, 1, 0)
        else:
            lax.fori_loop(0, 2, body, 0)
            hidden_send(k, 0, 1)
            hidden_send(k, 1, 0)

    def relay_up(k):
        comm.arrive(("hP", k, 0), hs(k, dn, 0))
        comm.send(("fP", k), hs(k, dn, 0), hs(k, dn, 0), YP)

    def relay_down(k):
        comm.arrive(("hM", k, 1), hs(k, up, 1))
        comm.send(("fM", k), hs(k, up, 1), hs(k, up, 1), YM)

    def relay(k):
        relay_up(k)
        relay_down(k)

    def h_ready(k):
        h, j = seq[k]
        comm.arrive(("h", k), hb.at[h, 0, :, pl.ds(j * FC, FC)])

    def far_ready(k):
        h, j = seq[k]
        comm.arrive(("f", k), hb.at[h, 0, :, pl.ds(j * FC, FC)])

    def project(h, acc, n, start, count, j0, j1, cols=slice(None), first=False):
        lo, depth = j0 * FC, (j1 - j0) * FC

        def body(i, carry):
            rows = pl.ds(pl.multiple_of(i * T2, T2), T2)
            total = None
            for b in range(count):
                yy = (start + b) % ny
                base = yy * FH + lo
                if not isinstance(base, int):
                    base = pl.multiple_of(base, FC)
                d = jnp.dot(hb[h, yy, rows, lo : lo + depth], w2b[n, pl.ds(base, depth), cols], preferred_element_type=jnp.float32)
                total = d if total is None else total + d
            acc[n, rows, cols] = total if first else acc[n, rows, cols] + total
            return carry

        lax.fori_loop(0, 2, body, 0)

    def partial_send(p):
        n, lo, size = pieces[p]
        comm.send(("y", p), y0.at[n, :, pl.ds(lo, size)], yr.at[n, :, pl.ds(lo, size)], PX)

    def early(p):
        n, lo, size = pieces[p]
        w2_ready(p)
        project(0, y0, n, xf + 1, ny - 1, 0, CHUNKS, slice(lo, lo + size), first=True)

    def late(p):
        n, lo, size = pieces[p]
        w2_far_ready(p)
        project(0, y0, n, xf, 1, 0, CHUNKS, slice(lo, lo + size))
        partial_send(p)

    def x_relay(quarter):
        comm.arrive(("xp", quarter), xq(0, y, quarter))
        comm.send(("x0P", quarter), xq(0, y, quarter), xq(0, y, quarter), YP)
        comm.send(("x0M", quarter), xq(0, y, quarter), xq(0, y, quarter), YM)

    def x_up(quarter):
        comm.arrive(("x0P", quarter), xq(0, dn, quarter))
        comm.send(("x0p", quarter), xq(0, dn, quarter), xq(0, dn, quarter), YP)

    def x_down(quarter):
        comm.arrive(("x0M", quarter), xq(0, up, quarter))
        comm.send(("x0m", quarter), xq(0, up, quarter), xq(0, up, quarter), YM)

    x_relay(0)
    for yk, dev in (("P", YP), ("M", YM), ("F", YF)):
        comm.send(("g" + yk,), gamma_ref, gb.at[y], dev)
    local_copy("g", gamma_ref, gb.at[y])
    x_relay(2)
    for p in range(NW):
        comm.send(("w1c", 0, p), w1_src(g, p), w1_dst(p, x, c), PC)
        local_copy(("w1", p), w1_src(g, p), w1_dst(p, x, c))
    x_up(0)
    x_relay(1)
    x_down(2)
    x_relay(3)
    w_from_inner("w1", w1_dst, 0)
    w_from_inner("w1", w1_dst, 1)
    w_from_pair("w1", w1_dst, 0)
    x_up(1)
    comm.send(("eP",), xl(0, dn, 0), xl(1, dn, 0), PX)
    comm.arrive(("x1P",), xl(1, dn, 1))
    comm.send(("x1p",), xs(1, dn, T2, T2 - T8), xs(1, dn, T2, T2 - T8), YP)
    w_from_pair("w1", w1_dst, 1)
    w1_inner(4)
    x_down(3)
    comm.send(("eM",), xl(0, up, 1), xl(1, up, 1), PX)
    comm.arrive(("x1M",), xl(1, up, 0))
    comm.send(("x1m",), xs(1, up, 0, T2 - T8), xs(1, up, 0, T2 - T8), YM)
    w_from_inner("w1", w1_dst, 2)
    w_from_inner("w1", w1_dst, 3)
    w_from_far("w1", w1_dst, 0)
    w_from_pair("w1", w1_dst, 2)
    w_from_far("w1", w1_dst, 1)

    local_wait("g", gb.at[y])
    comm.arrive(("g",), gb.at[pl.ds(0, ny - 1)])
    comm.arrive(("x0",), xl_all(0))
    x_load("near", 0, (y, up, dn))
    comm.arrive(("x0f",), xl_all(0))
    x_load("far", 0, (far,))
    for first in (T2 - T8, T - T8):
        comm.send(("eF", first), xs(0, far, first, T8), xs(1, far, first, T8), PX)
    for p in range(NP):
        comm.send(("w2x", p), w2_src(1 - g, p), w2_dst(p, x, c), PX)
    x_loaded("near", 0, ny - 1)
    x_loaded("far", 0, 1)
    norm()
    w1_ready(0)
    w1_ready(1)
    hidden(0)
    for p in range(NP):
        comm.send(("w2c", 0, p), w2_src(g, p), w2_dst(p, x, c), PC)
        local_copy(("w2", p), w2_src(g, p), w2_dst(p, x, c))
    w_from_pair("w1", w1_dst, 3)
    w1_inner(5)
    w_from_inner("w1", w1_dst, 4)
    w_from_far("w1", w1_dst, 2)
    relay(0)
    w1_ready(2)
    hidden(1)
    w_from_pair("w1", w1_dst, 4)
    w_from_pair("w1", w1_dst, 5)
    w2_inner(0)
    w2_inner(1)
    w_from_far("w1", w1_dst, 3)
    w1_ready(3)
    hidden(2)
    w_from_inner("w1", w1_dst, 5)
    relay(1)
    w_from_far("w1", w1_dst, 4)
    w_from_far("w1", w1_dst, 5)
    w1_ready(4)
    w1_ready(5)
    hidden(3)
    relay(2)
    comm.arrive(("x1",), xland.at[1, pl.ds(0, 2)])
    local_copy(("z", 1, "near"), x_ref, zb.at[y])
    x_load("near", 1, (up, dn, far))
    x_loaded("near", 1, ny)
    norm()
    hidden(4)
    w_from_pair("w2", w2_dst, 0)
    w_from_pair("w2", w2_dst, 1)
    w2_inner(2)
    relay(3)
    hidden(5)
    w_from_inner("w2", w2_dst, 0)
    w_from_far("w2", w2_dst, 0)
    w_from_pair("w2", w2_dst, 2)
    w2_inner(3)
    relay(4)
    w_from_inner("w2", w2_dst, 1)
    for k in range(4):
        h_ready(k)
    for k in range(3):
        far_ready(k)
    w2_ready(0)
    w2_far_ready(0)
    w_from_far("w2", w2_dst, 1)
    w2_ready(1)
    w2_far_ready(1)
    project(0, y0, 0, dn, ny - 1, 0, CHUNKS, first=True)
    project(0, y0, 0, far, 1, 0, CHUNKS - 1)
    far_ready(3)
    project(0, y0, 0, far, 1, CHUNKS - 1, CHUNKS)
    partial_send(0)
    partial_send(1)
    w_from_pair("w2", w2_dst, 3)
    w2_inner(4)
    w_from_pair("w2", w2_dst, 4)
    hidden(6)
    w_from_inner("w2", w2_dst, 2)
    relay(5)
    hidden(7)
    local_copy("xres", x_ref, zb.at[0])
    h_ready(4)
    far_ready(4)
    project(1, y1, 0, 0, ny, 0, 1, first=True)
    w_from_far("w2", w2_dst, 2)
    early(2)
    late(2)
    w_from_inner("w2", w2_dst, 3)
    relay(6)
    early(3)
    w_from_far("w2", w2_dst, 3)
    late(3)
    h_ready(5)
    far_ready(5)
    project(1, y1, 0, 0, ny, 1, 2)
    w_from_inner("w2", w2_dst, 4)
    early(4)
    relay(7)
    w_from_far("w2", w2_dst, 4)
    late(4)
    project(1, y1, 1, 0, ny, 0, 2, first=True)
    h_ready(6)
    h_ready(7)
    for n in (0, 1):
        project(1, y1, n, dn, ny - 1, 2, 4)
    far_ready(6)
    for n in (0, 1):
        project(1, y1, n, far, 1, 2, 3)
    local_wait("xres", zb.at[0])
    comm.arrive(("y",), yr)
    for n in (0, 1):
        y1[n] = y1[n] + yr[n] + zb[0, :, 2 * n * NC : 2 * (n + 1) * NC].astype(jnp.float32)
    far_ready(7)
    for n in (0, 1):
        cols = pl.ds(2 * n * NC, 2 * NC)
        base = pl.multiple_of(far * FH + 3 * FC, FC)
        for half in (0, 1):
            rows = slice(half * T2, (half + 1) * T2)
            last = jnp.dot(hb[1, far, rows, 3 * FC :], w2b[n, pl.ds(base, FC), :], preferred_element_type=jnp.float32)
            zb[1, rows, 2 * n * NC : 2 * (n + 1) * NC] = (y1[n, rows, :] + last).astype(jnp.bfloat16)
            local_copy("out", zb.at[1, tok(half), cols], out_ref.at[tok(half), cols])
    local_wait("out", out_ref)
    comm.finish("x", xland.at[:, :, pl.ds(0, T * 7 // 8), :])
    comm.finish("w1", w1b.at[:, pl.ds(0, (2 * nx - 1) * KR), :])
    comm.finish("w2", w2b.at[:, pl.ds(0, (2 * nx - 1) * RH), :])
    comm.finish("h", hb.at[:, pl.ds(0, ny - 1)])
    comm.finish("y", y0)
    comm.finish("g", gb.at[pl.ds(0, ny - 1)])
    assert len(comm.recv_ids) == N_RECV and len(comm.send_ids) == N_SEND and len(local) == N_LOCAL, (len(comm.recv_ids), len(comm.send_ids), len(local))


def solution(mesh):
    nx, ny = mesh.shape["row"] // 2, mesh.shape["col"]
    act_spec = P(None, ("dp", "row"), "col")

    def per_device(x_blk, gamma_blk, w_in_blk, w_out_blk):
        mbs, toks, D = x_blk.shape
        T = mbs * toks
        KR, FL = w_in_blk.shape
        R2, N = w_out_blk.shape
        bf16, f32 = jnp.bfloat16, jnp.float32
        any_spec = pl.BlockSpec(memory_space=pl.ANY)
        vmem_spec = pl.BlockSpec(memory_space=pltpu.VMEM)
        NC = N // CHUNKS
        flops = 2 * 2 * T * (ny * D) * (FL // 2) * 2
        out, _ = pl.pallas_call(
            functools.partial(kernel, nx, ny),
            out_shape=(jax.ShapeDtypeStruct((T, N), bf16), jax.ShapeDtypeStruct((2, ny, T, D), bf16)),
            in_specs=[any_spec, vmem_spec, any_spec, any_spec],
            out_specs=(any_spec, any_spec),
            scratch_shapes=[
                pltpu.VMEM((ny, T, D), bf16),
                pltpu.VMEM((CHUNKS, 2 * nx * KR, FL // 2 // CHUNKS), bf16),
                pltpu.VMEM((2, nx * R2, 2 * NC), bf16),
                pltpu.VMEM((2, ny, T, FL // 2), bf16),
                pltpu.VMEM((2, T, 2 * NC), f32),
                pltpu.VMEM((2, T, 2 * NC), f32),
                pltpu.VMEM((2, T, 2 * NC), f32),
                pltpu.VMEM((ny, 1, D), f32),
                pltpu.SemaphoreType.DMA((N_SEND,)),
                pltpu.SemaphoreType.DMA((N_RECV,)),
                pltpu.SemaphoreType.DMA((N_LOCAL,)),
            ],
            compiler_params=pltpu.CompilerParams(collective_id=0, has_side_effects=True, vmem_limit_bytes=67043328),
            cost_estimate=pl.CostEstimate(flops=flops, bytes_accessed=64 * T * D, transcendentals=T * FL),
            name="ln_mlp",
        )(x_blk.reshape(T, D), gamma_blk.reshape(1, D), w_in_blk, w_out_blk)
        return out.reshape(x_blk.shape)

    return jax.shard_map(per_device, mesh=mesh, in_specs=(act_spec, P("col"), P("row", "col"), P("row", "col")), out_specs=act_spec, check_vma=False)
```
